128 devices in a mesh: sample: 2 (over core), slab: 64 (over z, y, x).
Axes of the slice: x: 4, y: 4, z: 4, core: 2. Of those that a mesh axis runs over, the one named last changes fastest.
Arguments:
- force: float32 [3, 256, 32, 256], P(None, 'slab', None, 'sample'), parts along dimension 3, may hold values from -8 to 8, as said below
- modulus: float32 [256, 32, 256], P('slab', None, 'sample'), parts along dimension 2, may hold values from 0.2 to 1
Outputs:
- fine_field: float32 [3, 256, 32, 256], P(None, 'slab', None, 'sample'), parts along dimension 3
- coarse_field: float32 [3, 128, 16, 128], P(None, 'slab', None, 'sample'), parts along dimension 3
- compliance: float32 [4], P('sample'), parts along dimension 0
The draws below stay inside these ranges and needn't reach their ends.
There are 2 independent parts, one for each index of `sample`. The reference program is written for one: setup_inputs(seed, part) draws one part's arguments, and reference() takes and returns one part's arrays. A program takes and returns all parts, laid end to end along the dimension named above; each array names one. Nothing has to cross between parts.
Inputs may be any that keep to these rules, and one draw needn't show every extreme that they name: Body force on each cell and component.
All inputs are finite; a program needn't handle non-finite values.
Results may differ from the reference program's by a relative error of at most 0.0001.
Values sent between devices are 32-bit elements; how exact they have to be, the bound alone decides.
No kernel may reach another device: no remote copies, remote signals or barrier semaphores. Data moves between devices by JAX's collectives and lax.ppermute only.
A program may use at most 128 MiB of HBM per device.

```python
import math
import jax
import jax.numpy as jnp
from jax import lax

NX = 128
NY = 32
ITERS = 2
SMOOTH = 2
CDEG = 4
NZ = 256


def draw_force(key, part):
    noise_key = jax.random.fold_in(key, 11)
    depth = jnp.arange(NZ, dtype=jnp.float32) / float(max(NZ - 1, 1))
    ramp = (0.5 + 1.5 * depth)[None, :, None, None]
    base = jax.random.truncated_normal(noise_key, -4.0, 4.0, (3, NZ, NY, NX), jnp.float32)
    return (base * ramp).astype(jnp.float32)


def block_levels(rng, shape, pieces, smallest, largest):
    def one(dim, parts):
        steps = jax.random.uniform(jax.random.fold_in(jax.random.fold_in(rng, 6), dim), (parts,), jnp.float32, smallest / len(pieces), largest / len(pieces))
        return jnp.repeat(jnp.exp(steps), shape[dim] // parts).reshape((-1,) + (1,) * (len(shape) - dim - 1))

    factor_of = one(*pieces[0])
    for cut in pieces[1:]:
        factor_of = factor_of * one(*cut)
    return factor_of


def setup_inputs(seed: int = 0, part: int = 0) -> dict:
    arg_keys = jax.random.split(jax.random.key(seed), 3)
    own_keys = jax.random.split(jax.random.fold_in(arg_keys[2], part), 3)
    return {
        "force": draw_force(jax.random.fold_in(jax.random.fold_in(arg_keys[2], part), 71), part),
        "modulus": jnp.clip(jnp.exp(math.log(1.0) - 1.609438 * jax.random.uniform(own_keys[1], (NZ, NY, NX), jnp.float32) ** block_levels(own_keys[1], (NZ, NY, NX), ((0, 64),), -0.2, 0.2)), 0.2, 1.0),
    }


def shift_back(values, dimension):
    length = values.shape[dimension]
    zeroes = jnp.zeros_like(lax.slice_in_dim(values, 0, 1, axis=dimension))
    return jnp.concatenate([zeroes, lax.slice_in_dim(values, 0, length - 1, axis=dimension)], axis=dimension)


def shift_ahead(values, dimension):
    length = values.shape[dimension]
    zeroes = jnp.zeros_like(lax.slice_in_dim(values, 0, 1, axis=dimension))
    return jnp.concatenate([lax.slice_in_dim(values, 1, length, axis=dimension), zeroes], axis=dimension)


def operate(displace, lame):
    grad_z = shift_ahead(displace, 1) - displace
    grad_y = shift_ahead(displace, 2) - displace
    grad_x = shift_ahead(displace, 3) - displace
    spread = lame * (grad_x[0] + grad_y[1] + grad_z[2])
    flux_z = lame * grad_z
    flux_y = lame * grad_y
    flux_x = lame * grad_x
    result = (shift_back(flux_z, 1) - flux_z) + (shift_back(flux_y, 2) - flux_y) + (shift_back(flux_x, 3) - flux_x)
    pressure = jnp.stack([shift_back(spread, 2) - spread, shift_back(spread, 1) - spread, shift_back(spread, 0) - spread])
    return result + pressure


def diag_inverse(lame):
    laplace = (lame + shift_back(lame, 0)) + (lame + shift_back(lame, 1)) + (lame + shift_back(lame, 2))
    diagonal = jnp.stack([laplace + lame + shift_back(lame, 2), laplace + lame + shift_back(lame, 1), laplace + lame + shift_back(lame, 0)])
    return 1.0 / diagonal


def restrict_scalar(values):
    shape = values.shape
    return values.reshape(shape[0] // 2, 2, shape[1] // 2, 2, shape[2] // 2, 2).mean(axis=(1, 3, 5))


def restrict_vector(values):
    shape = values.shape
    return values.reshape(shape[0], shape[1] // 2, 2, shape[2] // 2, 2, shape[3] // 2, 2).mean(axis=(2, 4, 6))


def prolong(values):
    return jnp.repeat(jnp.repeat(jnp.repeat(values, 2, 1), 2, 2), 2, 3)


def chebyshev(iterate, residue, operator, inverse, degree, low_end, high_end):
    centre = (high_end + low_end) / 2.0
    half_width = (high_end - low_end) / 2.0
    spread_ratio = centre / half_width
    rho_now = 1.0 / spread_ratio
    update = inverse * residue / centre
    for section in range(degree):
        iterate = iterate + update
        residue = residue - operator(update)
        if section + 1 < degree:
            rho_next = 1.0 / (2.0 * spread_ratio - rho_now)
            update = rho_next * rho_now * update + (2.0 * rho_next / half_width) * (inverse * residue)
            rho_now = rho_next
    return iterate, residue


def reference(force, modulus):
    lame = 0.4 * modulus
    coarse_lame = restrict_scalar(lame)
    fine_inverse = diag_inverse(lame)
    coarse_inverse = diag_inverse(coarse_lame)

    def fine_operator(vector):
        return operate(vector, lame)

    def coarse_operator(vector):
        return operate(vector, coarse_lame)

    iterate = jnp.zeros_like(force)
    residue = force
    for cycle in range(ITERS):
        iterate, residue = chebyshev(iterate, residue, fine_operator, fine_inverse, SMOOTH, 0.25, 2.0)
        coarse_rhs = 4.0 * restrict_vector(residue)
        correction, unused = chebyshev(jnp.zeros_like(coarse_rhs), coarse_rhs, coarse_operator, coarse_inverse, CDEG, 0.02, 2.0)
        expanded = prolong(correction)
        iterate = iterate + expanded
        residue = residue - fine_operator(expanded)
        iterate, residue = chebyshev(iterate, residue, fine_operator, fine_inverse, SMOOTH, 0.25, 2.0)
    coarse_force = restrict_vector(force)
    coarse_field, unused = chebyshev(jnp.zeros_like(coarse_force), 4.0 * coarse_force, coarse_operator, coarse_inverse, 2 * CDEG, 0.02, 2.0)
    cells = float(NX * NY * NZ)
    compliance = jnp.stack([jnp.sum(force * iterate) / cells, jnp.sum(coarse_force * coarse_field) / (cells / 8.0)])
    return iterate, coarse_field, compliance
```

```python
import math

import jax
import jax.numpy as jnp
from jax import lax
from jax.experimental import pallas as pl
from jax.experimental.pallas import tpu as pltpu
from jax.sharding import PartitionSpec as P

ITERS = 2
SMOOTH = 2
CDEG = 4
FINE = (0.25, 2.0)
COARSE = (0.02, 2.0)


def coefficients(low_end, high_end, degree):
    centre = (high_end + low_end) / 2.0
    half = (high_end - low_end) / 2.0
    ratio = centre / half
    rho = 1.0 / ratio
    steps = []
    for _ in range(degree - 1):
        after = 1.0 / (2.0 * ratio - rho)
        steps.append((after * rho, 2.0 * after / half))
        rho = after
    return 1.0 / centre, steps, ratio


FIRST_F, STEPS_F, _ = coefficients(*FINE, SMOOTH)
FIRST_C, STEPS_C, RATIO_C = coefficients(*COARSE, 2 * CDEG)


def lanes(shape):
    return lax.broadcasted_iota(jnp.int32, shape, len(shape) - 1)


def ahead(v, axis, by=1):
    n = v.shape[axis]
    at = lax.broadcasted_iota(jnp.int32, v.shape, axis)
    return jnp.where(at < n - by, pltpu.roll(v, n - by, axis), 0.0)


def back(v, axis, by=1):
    at = lax.broadcasted_iota(jnp.int32, v.shape, axis)
    return jnp.where(at >= by, pltpu.roll(v, by, axis), 0.0)


def operate(u, m, step):
    low = [c[:-1] for c in u]
    gz = [c[1:] - l for c, l in zip(u, low)]
    gx0 = ahead(low[0], 2, step) - low[0]
    gy1 = ahead(low[1], 1) - low[1]
    s = m * (gx0 + gy1 + gz[2])
    inner = m[1:]
    si = s[1:]
    out = []
    for c in range(3):
        here = low[c][1:]
        fx = inner * (gx0[1:] if c == 0 else ahead(here, 2, step) - here)
        fy = inner * (gy1[1:] if c == 1 else ahead(here, 1) - here)
        fz = m * gz[c]
        if c == 0:
            fx = fx + si
        elif c == 1:
            fy = fy + si
        else:
            fz = fz + s
        out.append((fz[:-1] - fz[1:]) + (back(fy, 1) - fy) + (back(fx, 2, step) - fx))
    return out


def inverse(m, step):
    here = m[1:]
    below = m[:-1]
    by = back(here, 1)
    bx = back(here, 2, step)
    lap = (here + below) + (here + by) + (here + bx) + here
    inside = here > 0.0
    return [
        jnp.where(inside, 1.0 / jnp.where(inside, lap + d, 1.0), 0.0) for d in (bx, by, below)
    ]


def trim(v, n=1):
    return v[n : v.shape[0] - n]


def halve_rows(tmp, v):
    k, rows, _ = v.shape
    tmp[0:k] = v
    return tmp[0:k, pl.ds(0, rows // 2, stride=2), :] + tmp[0:k, pl.ds(1, rows // 2, stride=2), :]


def pack(even_sum, odd_sum):
    even = lanes(even_sum.shape) % 2 == 0
    ax = even_sum.ndim - 1
    near = jnp.where(even, even_sum, odd_sum)
    far = jnp.where(even, pltpu.roll(even_sum, 127, ax), pltpu.roll(odd_sum, 1, ax))
    return near + far


def pair_layers(v):
    return jnp.concatenate([v[i : i + 1] + v[i + 1 : i + 2] for i in range(0, v.shape[0], 2)], 0)


def spread(tmp, e):
    k, rows, _ = e.shape
    even = lanes(e.shape) % 2 == 0
    both = jnp.where(even, e, pltpu.roll(e, 1, 2))
    tmp[0:k, pl.ds(0, rows, stride=2), :] = both
    tmp[0:k, pl.ds(1, rows, stride=2), :] = both
    return tmp[0:k]


def layers(v, order):
    return jnp.concatenate([v[i : i + 1] for i in order], 0)


def by_side(flag, put, a, b):
    lower = flag == 0

    @pl.when(lower)
    def _():
        put(a, b)

    @pl.when(jnp.logical_not(lower))
    def _():
        put(b, a)


def first_kernel(par, f_ref, e_ref, a_ref, b_ref, x_ref, big_ref, small_ref, fe, me, tmp):
    for c in range(3):
        fe[c, 2:6] = f_ref[c]
    me[3:7] = 0.4 * e_ref[...]

    def take(up, down):
        for c in range(3):
            fe[c, 6:8] = up[2 * c : 2 * c + 2]
            fe[c, 0:2] = down[2 * c : 2 * c + 2]
        me[7:9] = 0.4 * up[6:8]
        me[0:3] = 0.4 * down[6:9]

    by_side(par[0], take, a_ref, b_ref)
    m = me[...]
    p = inverse(m, 1)
    r = [fe[c] for c in range(3)]
    w = [p[c] * r[c] * FIRST_F for c in range(3)]
    aw = operate(w, m[1:8], 1)
    r = [trim(r[c]) - aw[c] for c in range(3)]
    now, gain = STEPS_F[0]
    w2 = [now * trim(w[c]) + gain * (trim(p[c]) * r[c]) for c in range(3)]
    aw = operate(w2, m[2:7], 1)
    for c in range(3):
        x_ref[c] = w[c][2:6] + w2[c][1:5]
        done = trim(r[c]) - aw[c]
        big_ref[4 * c : 4 * c + 4] = done
        rc = halve_rows(tmp, pair_layers(done)) * 0.5
        fc = halve_rows(tmp, pair_layers(fe[c, 2:6])) * 0.5
        both = pack(rc, fc)
        small_ref[2 * c : 2 * c + 2] = both
        big_ref[17 + c, 0:16] = both[0]
        big_ref[17 + c, 16:32] = both[1]
    big_ref[12:17] = m[2:7]
    cm = halve_rows(tmp, pair_layers(m[1:7])) * 0.125
    cm = pack(cm, cm)
    small_ref[6:9] = cm
    big_ref[20, 0:16] = cm[0]
    big_ref[20, 16:32] = cm[1]
    big_ref[21, 0:16] = cm[2]
    big_ref[21, 16:32] = cm[2]


def second_kernel(
    par, f_ref, x_ref, mine, own, a1, b1, a2, b2, a3, b3,
    xo_ref, ro_ref, send_a, send_b, small_ref, mo_ref, cmo_ref, xc_ref, rc_ref, sum_ref,
    re, me, cf, cm, tmp,
):
    for c in range(3):
        re[c, 4:8] = mine[4 * c : 4 * c + 4]
        cf[c, 6:8] = own[2 * c : 2 * c + 2]
    me[5:9] = mine[13:17]
    cm[7:9] = own[7:9]

    def near(up, down):
        for c in range(3):
            re[c, 8:12] = up[4 * c : 4 * c + 4]
            re[c, 0:4] = down[4 * c : 4 * c + 4]
            for j in range(2):
                cf[c, 8 + j] = up[17 + c, 16 * j : 16 * j + 16]
                cf[c, 4 + j] = down[17 + c, 16 * j : 16 * j + 16]
        me[9:13] = up[13:17]
        me[0:5] = down[12:17]
        cm[9] = up[20, 16:32]
        cm[10] = up[21, 0:16]
        cm[5] = down[20, 16:32]
        cm[6] = down[21, 0:16]

    def second(up, down):
        for c in range(3):
            cf[c, 10:12] = up[2 * c : 2 * c + 2]
            cf[c, 2:4] = down[2 * c : 2 * c + 2]
        cm[11:13] = up[7:9]
        cm[3:5] = down[7:9]

    def third(up, down):
        for c in range(3):
            cf[c, 12:14] = up[2 * c : 2 * c + 2]
            cf[c, 0:2] = down[2 * c : 2 * c + 2]
        cm[13:15] = up[7:9]
        cm[0:3] = down[6:9]

    by_side(par[0], near, a1, b1)
    by_side(par[1], second, a2, b2)
    by_side(par[2], third, a3, b3)

    mc = cm[...]
    pc = inverse(mc, 2)
    r = [cf[c] for c in range(3)]
    w = [pc[c] * r[c] * FIRST_C for c in range(3)]
    e = [w[c][3:11] for c in range(3)]
    xc = [w[c][6:8] for c in range(3)]
    part = None
    for k in range(1, 7):
        aw = operate(w, mc[k : 15 - k], 2)
        r = [trim(r[c]) - aw[c] for c in range(3)]
        now, gain = STEPS_C[k - 1]
        if k == 4:
            odd = lanes((2, 16, 128)) % 2 == 1
            part = sum(
                jnp.sum(jnp.where(odd, xc[c] * (cf[c, 6:8] + r[c][2:4]), 0.0)) for c in range(3)
            )
        w = [now * trim(w[c]) + gain * (pc[c][k : 14 - k] * r[c]) for c in range(3)]
        if k <= 3:
            e = [e[c] + w[c][3 - k : 11 - k] for c in range(3)]
        xc = [xc[c] + w[c][6 - k : 8 - k] for c in range(3)]
    for c in range(3):
        xc_ref[c] = xc[c]
        rc_ref[c] = r[c]
    last = w

    m = me[...]
    order = [0] + [i for i in range(1, 7) for _ in range(2)] + [7]
    v = [layers(spread(tmp, e[c]), order) for c in range(3)]
    aw = operate(v, m, 1)
    p = inverse(m, 1)
    r = [re[c] - aw[c] for c in range(3)]
    now, gain = STEPS_F[0]
    w = [p[c] * r[c] * FIRST_F for c in range(3)]
    x = [x_ref[c] + v[c][5:9] + w[c][4:8] for c in range(3)]
    aw = operate(w, m[1:12], 1)
    r = [trim(r[c]) - aw[c] for c in range(3)]
    w = [now * trim(w[c]) + gain * (p[c][1:11] * r[c]) for c in range(3)]
    x = [x[c] + w[c][3:7] for c in range(3)]
    aw = operate(w, m[2:11], 1)
    r = [trim(r[c]) - aw[c] for c in range(3)]
    whole = sum(jnp.sum(x[c] * (f_ref[c] + r[c][2:6])) for c in range(3))
    w = [p[c][2:10] * r[c] * FIRST_F for c in range(3)]
    x = [x[c] + w[c][2:6] for c in range(3)]
    aw = operate(w, m[3:10], 1)
    r = [trim(r[c]) - aw[c] for c in range(3)]
    w = [now * trim(w[c]) + gain * (p[c][3:9] * r[c]) for c in range(3)]
    aw = operate(w, m[4:9], 1)
    for c in range(3):
        xo_ref[c] = x[c] + w[c][1:5]
        done = trim(r[c]) - aw[c]
        ro_ref[c] = done
        rc = halve_rows(tmp, pair_layers(done)) * 0.5
        at = lanes(rc.shape) % 2 == 0
        both = jnp.where(at, rc + pltpu.roll(rc, 127, 2), last[c])
        small_ref[2 * c : 2 * c + 2] = both
        for ref in (send_a, send_b):
            ref[3 + c, 0:16] = both[0]
            ref[3 + c, 16:32] = both[1]
    for c in range(3):
        send_a[c] = ro_ref[c, 3 - 3 * par[0]]
        send_b[c] = ro_ref[c, 3 * par[0]]
    mo_ref[...] = m[3:10]
    cmo_ref[...] = mc[2:13]
    at = lanes((1, 128))
    sum_ref[...] = jnp.where(at == 0, whole, 0.0) + jnp.where(at == 1, part, 0.0)


def third_kernel(
    par, x_ref, r_ref, own, m_ref, cm_ref, xc_ref, rc_ref, a1, b1, a2, b2,
    out_ref, coarse_ref, re, cf, tmp,
):
    for c in range(3):
        re[c, 1:5] = r_ref[c]
        cf[c, 4:6] = own[2 * c : 2 * c + 2]

    def near(up, down):
        for c in range(3):
            re[c, 5] = up[c]
            re[c, 0] = down[c]
            for j in range(2):
                cf[c, 6 + j] = up[3 + c, 16 * j : 16 * j + 16]
                cf[c, 2 + j] = down[3 + c, 16 * j : 16 * j + 16]

    def second(up, down):
        for c in range(3):
            cf[c, 8:10] = up[2 * c : 2 * c + 2]
            cf[c, 0:2] = down[2 * c : 2 * c + 2]

    by_side(par[0], near, a1, b1)
    by_side(par[1], second, a2, b2)

    mc = cm_ref[...]
    pc = inverse(mc, 2)

    def either(shape, a, b):
        return jnp.where(lanes(shape) % 2 == 0, a, b)

    r = [cf[c] for c in range(3)]
    w = [either(r[c].shape, pc[c] * r[c] * FIRST_C, r[c]) for c in range(3)]
    r = [
        jnp.concatenate([r[c][0:4], either((2, 16, 128), r[c][4:6], rc_ref[c]), r[c][6:10]], 0)
        for c in range(3)
    ]
    e = [w[c][3:7] for c in range(3)]
    for k in range(1, 4):
        aw = operate(w, mc[k : 11 - k], 2)
        r = [trim(r[c]) - aw[c] for c in range(3)]
        now, gain = STEPS_C[k - 1]
        if k == 1:
            line = (1, 1, 128)
            now = either(line, now, STEPS_C[6][0])
            gain = either(line, gain, STEPS_C[6][1])
        w = [now * trim(w[c]) + gain * (pc[c][k : 10 - k] * r[c]) for c in range(3)]
        if k == 1:
            col = lax.broadcasted_iota(jnp.int32, (128, 64), 1)
            row = lax.broadcasted_iota(jnp.int32, (128, 64), 0)
            pick = jnp.where(row == 2 * col + 1, 1.0, 0.0).astype(jnp.float32)
            for c in range(3):
                whole = (xc_ref[c] + w[c][3:5]).reshape(32, 128)
                coarse_ref[c] = jnp.dot(
                    whole, pick, precision=lax.Precision.HIGHEST, preferred_element_type=jnp.float32
                ).reshape(2, 16, 64)
        e = [e[c] + w[c][3 - k : 7 - k] for c in range(3)]

    m = m_ref[...]
    order = [0, 0, 1, 1, 2, 2, 3, 3]
    v = [layers(spread(tmp, e[c]), order) for c in range(3)]
    aw = operate(v, m, 1)
    p = inverse(m, 1)
    r = [re[c] - aw[c] for c in range(3)]
    now, gain = STEPS_F[0]
    w = [p[c] * r[c] * FIRST_F for c in range(3)]
    aw = operate(w, m[1:6], 1)
    for c in range(3):
        after = r[c][1:5] - aw[c]
        out_ref[c] = x_ref[c] + v[c][2:6] + (1.0 + now) * w[c][1:5] + gain * (p[c][1:5] * after)


def call(kernel, outs, scratch, par, *args, flops=1 << 22):
    return pl.pallas_call(
        kernel,
        out_shape=[jax.ShapeDtypeStruct(s, jnp.float32) for s in outs],
        in_specs=[pl.BlockSpec(memory_space=pltpu.SMEM)]
        + [pl.BlockSpec(memory_space=pltpu.VMEM)] * len(args),
        out_specs=[pl.BlockSpec(memory_space=pltpu.VMEM)] * len(outs),
        scratch_shapes=[pltpu.VMEM(s, jnp.float32) for s in scratch],
        cost_estimate=pl.CostEstimate(flops=flops, bytes_accessed=1 << 20, transcendentals=0),
    )(par, *args)


def swap(x, axis, distance, second):
    n = lax.axis_size(axis)
    pairs = []
    for i in range(n - distance):
        if (i // distance) % 2 == second:
            pairs += [(i, i + distance), (i + distance, i)]
    return lax.ppermute(x, axis, pairs)


def body(force, modulus):
    me = lax.axis_index("slab")
    par = jnp.stack([me % 2, (me // 2) % 2, (me // 3) % 2]).astype(jnp.int32)
    odd = me % 2

    def edge(side):
        f = lax.dynamic_slice_in_dim(force, 2 - 2 * side, 2, 1).reshape(6, 32, 128)
        return jnp.concatenate([f, lax.dynamic_slice_in_dim(modulus, 1 - side, 3, 0)], 0)

    a = swap(edge(odd), "slab", 1, 0)
    b = swap(edge(1 - odd), "slab", 1, 1)
    x, big, small = call(
        first_kernel,
        [(3, 4, 32, 128), (22, 32, 128), (9, 16, 128)],
        [(3, 8, 32, 128), (9, 32, 128), (4, 32, 128)],
        par, force, modulus, a, b,
    )
    got = [swap(big, "slab", 1, 0), swap(big, "slab", 1, 1)]
    got += [swap(small, "slab", d, h) for d in (2, 3) for h in (0, 1)]
    x, r, send_a, send_b, small, m, cm, xc, rc, part = call(
        second_kernel,
        [
            (3, 4, 32, 128), (3, 4, 32, 128), (6, 32, 128), (6, 32, 128), (6, 16, 128),
            (7, 32, 128), (11, 16, 128), (3, 2, 16, 128), (3, 2, 16, 128), (1, 128),
        ],
        [(3, 12, 32, 128), (13, 32, 128), (3, 14, 16, 128), (15, 16, 128), (8, 32, 128)],
        par, force, x, big, small, *got,
    )
    n = lax.axis_size("slab")
    got = [swap(send_a, "slab", 1, 0), swap(send_b, "slab", 1, 1)]
    got += [swap(small, "slab", 2, h) for h in (0, 1)]
    sums = lax.all_to_all(jnp.broadcast_to(part[None], (n, 1, 128)), "slab", 0, 0, tiled=True)
    fine, coarse = call(
        third_kernel,
        [(3, 4, 32, 128), (3, 2, 16, 64)],
        [(3, 6, 32, 128), (3, 10, 16, 128), (4, 32, 128)],
        par, x, r, small, m, cm, xc, rc, *got,
    )
    cells = float(modulus.size * n)
    angle = math.acosh(RATIO_C)
    half = math.cosh(CDEG * angle)
    full = math.cosh(2 * CDEG * angle)
    scale = jnp.array([1.0 / cells, 2.0 * half * half / full / 4.0 / (cells / 8.0)], jnp.float32)
    return fine, coarse, sums.sum(axis=(0, 1))[:2] * scale


def solution(mesh):
    return jax.shard_map(
        body,
        mesh=mesh,
        in_specs=(P(None, "slab", None, "sample"), P("slab", None, "sample")),
        out_specs=(P(None, "slab", None, "sample"), P(None, "slab", None, "sample"), P("sample")),
        check_vma=False,
    )
```

```python
import math

import jax
import jax.numpy as jnp
from jax import lax
from jax.experimental import pallas as pl
from jax.experimental.pallas import tpu as pltpu
from jax.sharding import PartitionSpec as P

ITERS = 2
SMOOTH = 2
CDEG = 4
FINE = (0.25, 2.0)
COARSE = (0.02, 2.0)


def coefficients(low_end, high_end, degree):
    centre = (high_end + low_end) / 2.0
    half = (high_end - low_end) / 2.0
    ratio = centre / half
    rho = 1.0 / ratio
    steps = []
    for _ in range(degree - 1):
        after = 1.0 / (2.0 * ratio - rho)
        steps.append((after * rho, 2.0 * after / half))
        rho = after
    return 1.0 / centre, steps, ratio


FIRST_F, STEPS_F, _ = coefficients(*FINE, SMOOTH)
FIRST_C, STEPS_C, RATIO_C = coefficients(*COARSE, 2 * CDEG)


def lanes(shape):
    return lax.broadcasted_iota(jnp.int32, shape, len(shape) - 1)


def ahead(v, axis, by=1):
    n = v.shape[axis]
    at = lax.broadcasted_iota(jnp.int32, v.shape, axis)
    return jnp.where(at < n - by, pltpu.roll(v, n - by, axis), 0.0)


def back(v, axis, by=1):
    at = lax.broadcasted_iota(jnp.int32, v.shape, axis)
    return jnp.where(at >= by, pltpu.roll(v, by, axis), 0.0)


def operate(u, m, step):
    low = [c[:-1] for c in u]
    gz = [c[1:] - l for c, l in zip(u, low)]
    gx0 = ahead(low[0], 2, step) - low[0]
    gy1 = ahead(low[1], 1) - low[1]
    s = m * (gx0 + gy1 + gz[2])
    inner = m[1:]
    si = s[1:]
    out = []
    for c in range(3):
        here = low[c][1:]
        fx = inner * (gx0[1:] if c == 0 else ahead(here, 2, step) - here)
        fy = inner * (gy1[1:] if c == 1 else ahead(here, 1) - here)
        fz = m * gz[c]
        if c == 0:
            fx = fx + si
        elif c == 1:
            fy = fy + si
        else:
            fz = fz + s
        out.append((fz[:-1] - fz[1:]) + (back(fy, 1) - fy) + (back(fx, 2, step) - fx))
    return out


def inverse(m, step):
    here = m[1:]
    below = m[:-1]
    by = back(here, 1)
    bx = back(here, 2, step)
    lap = (here + below) + (here + by) + (here + bx) + here
    inside = here > 0.0
    return [
        jnp.where(inside, 1.0 / jnp.where(inside, lap + d, 1.0), 0.0) for d in (bx, by, below)
    ]


def trim(v, n=1):
    return v[n : v.shape[0] - n]


def halve_rows(tmp, v):
    k, rows, _ = v.shape
    tmp[0:k] = v
    return tmp[0:k, pl.ds(0, rows // 2, stride=2), :] + tmp[0:k, pl.ds(1, rows // 2, stride=2), :]


def pack(even_sum, odd_sum):
    even = lanes(even_sum.shape) % 2 == 0
    ax = even_sum.ndim - 1
    near = jnp.where(even, even_sum, odd_sum)
    far = jnp.where(even, pltpu.roll(even_sum, 127, ax), pltpu.roll(odd_sum, 1, ax))
    return near + far


def pair_layers(v):
    return jnp.concatenate([v[i : i + 1] + v[i + 1 : i + 2] for i in range(0, v.shape[0], 2)], 0)


def spread(tmp, e):
    k, rows, _ = e.shape
    even = lanes(e.shape) % 2 == 0
    both = jnp.where(even, e, pltpu.roll(e, 1, 2))
    tmp[0:k, pl.ds(0, rows, stride=2), :] = both
    tmp[0:k, pl.ds(1, rows, stride=2), :] = both
    return tmp[0:k]


def layers(v, order):
    return jnp.concatenate([v[i : i + 1] for i in order], 0)


def by_side(flag, put, a, b):
    lower = flag == 0

    @pl.when(lower)
    def _():
        put(a, b)

    @pl.when(jnp.logical_not(lower))
    def _():
        put(b, a)


def first_kernel(par, f_ref, e_ref, a_ref, b_ref, x_ref, big_ref, small_ref, fe, me, tmp):
    for c in range(3):
        fe[c, 2:6] = f_ref[c]
    me[3:7] = 0.4 * e_ref[...]

    def take(up, down):
        for c in range(3):
            fe[c, 6:8] = up[2 * c : 2 * c + 2]
            fe[c, 0:2] = down[2 * c : 2 * c + 2]
        me[7:9] = 0.4 * up[6:8]
        me[0:3] = 0.4 * down[6:9]

    by_side(par[0], take, a_ref, b_ref)
    m = me[...]
    p = inverse(m, 1)
    r = [fe[c] for c in range(3)]
    w = [p[c] * r[c] * FIRST_F for c in range(3)]
    aw = operate(w, m[1:8], 1)
    r = [trim(r[c]) - aw[c] for c in range(3)]
    now, gain = STEPS_F[0]
    w2 = [now * trim(w[c]) + gain * (trim(p[c]) * r[c]) for c in range(3)]
    aw = operate(w2, m[2:7], 1)
    for c in range(3):
        x_ref[c] = w[c][2:6] + w2[c][1:5]
        done = trim(r[c]) - aw[c]
        big_ref[4 * c : 4 * c + 4] = done
        rc = halve_rows(tmp, pair_layers(done)) * 0.5
        fc = halve_rows(tmp, pair_layers(fe[c, 2:6])) * 0.5
        both = pack(rc, fc)
        small_ref[2 * c : 2 * c + 2] = both
        big_ref[17 + c, 0:16] = both[0]
        big_ref[17 + c, 16:32] = both[1]
    big_ref[12:17] = m[2:7]
    cm = halve_rows(tmp, pair_layers(m[1:7])) * 0.125
    cm = pack(cm, cm)
    small_ref[6:9] = cm
    big_ref[20, 0:16] = cm[0]
    big_ref[20, 16:32] = cm[1]
    big_ref[21, 0:16] = cm[2]
    big_ref[21, 16:32] = cm[2]


def second_kernel(
    par, f_ref, x_ref, mine, own, a1, b1, a2, b2, a3, b3,
    xo_ref, ro_ref, send_a, send_b, small_ref, mo_ref, cmo_ref, xc_ref, rc_ref, sum_ref,
    re, me, cf, cm, tmp,
):
    for c in range(3):
        re[c, 4:8] = mine[4 * c : 4 * c + 4]
        cf[c, 6:8] = own[2 * c : 2 * c + 2]
    me[5:9] = mine[13:17]
    cm[7:9] = own[7:9]

    def near(up, down):
        for c in range(3):
            re[c, 8:12] = up[4 * c : 4 * c + 4]
            re[c, 0:4] = down[4 * c : 4 * c + 4]
            for j in range(2):
                cf[c, 8 + j] = up[17 + c, 16 * j : 16 * j + 16]
                cf[c, 4 + j] = down[17 + c, 16 * j : 16 * j + 16]
        me[9:13] = up[13:17]
        me[0:5] = down[12:17]
        cm[9] = up[20, 16:32]
        cm[10] = up[21, 0:16]
        cm[5] = down[20, 16:32]
        cm[6] = down[21, 0:16]

    def second(up, down):
        for c in range(3):
            cf[c, 10:12] = up[2 * c : 2 * c + 2]
            cf[c, 2:4] = down[2 * c : 2 * c + 2]
        cm[11:13] = up[7:9]
        cm[3:5] = down[7:9]

    def third(up, down):
        for c in range(3):
            cf[c, 12:14] = up[2 * c : 2 * c + 2]
            cf[c, 0:2] = down[2 * c : 2 * c + 2]
        cm[13:15] = up[7:9]
        cm[0:3] = down[6:9]

    by_side(par[0], near, a1, b1)
    by_side(par[1], second, a2, b2)
    by_side(par[2], third, a3, b3)

    mc = cm[...]
    pc = inverse(mc, 2)
    r = [cf[c] for c in range(3)]
    w = [pc[c] * r[c] * FIRST_C for c in range(3)]
    e = [w[c][3:11] for c in range(3)]
    xc = [w[c][6:8] for c in range(3)]
    part = None
    for k in range(1, 7):
        aw = operate(w, mc[k : 15 - k], 2)
        r = [trim(r[c]) - aw[c] for c in range(3)]
        now, gain = STEPS_C[k - 1]
        if k == 4:
            odd = lanes((2, 16, 128)) % 2 == 1
            part = sum(
                jnp.sum(jnp.where(odd, xc[c] * (cf[c, 6:8] + r[c][2:4]), 0.0)) for c in range(3)
            )
        w = [now * trim(w[c]) + gain * (pc[c][k : 14 - k] * r[c]) for c in range(3)]
        if k <= 3:
            e = [e[c] + w[c][3 - k : 11 - k] for c in range(3)]
        xc = [xc[c] + w[c][6 - k : 8 - k] for c in range(3)]
    for c in range(3):
        xc_ref[c] = xc[c]
        rc_ref[c] = r[c]
    last = w

    m = me[...]
    order = [0] + [i for i in range(1, 7) for _ in range(2)] + [7]
    v = [layers(spread(tmp, e[c]), order) for c in range(3)]
    aw = operate(v, m, 1)
    p = inverse(m, 1)
    r = [re[c] - aw[c] for c in range(3)]
    now, gain = STEPS_F[0]
    w = [p[c] * r[c] * FIRST_F for c in range(3)]
    x = [x_ref[c] + v[c][5:9] + w[c][4:8] for c in range(3)]
    aw = operate(w, m[1:12], 1)
    r = [trim(r[c]) - aw[c] for c in range(3)]
    w = [now * trim(w[c]) + gain * (p[c][1:11] * r[c]) for c in range(3)]
    x = [x[c] + w[c][3:7] for c in range(3)]
    aw = operate(w, m[2:11], 1)
    r = [trim(r[c]) - aw[c] for c in range(3)]
    whole = sum(jnp.sum(x[c] * (f_ref[c] + r[c][2:6])) for c in range(3))
    w = [p[c][2:10] * r[c] * FIRST_F for c in range(3)]
    x = [x[c] + w[c][2:6] for c in range(3)]
    aw = operate(w, m[3:10], 1)
    r = [trim(r[c]) - aw[c] for c in range(3)]
    w = [now * trim(w[c]) + gain * (p[c][3:9] * r[c]) for c in range(3)]
    aw = operate(w, m[4:9], 1)
    for c in range(3):
        xo_ref[c] = x[c] + w[c][1:5]
        done = trim(r[c]) - aw[c]
        ro_ref[c] = done
        rc = halve_rows(tmp, pair_layers(done)) * 0.5
        at = lanes(rc.shape) % 2 == 0
        both = jnp.where(at, rc + pltpu.roll(rc, 127, 2), last[c])
        small_ref[2 * c : 2 * c + 2] = both
        for ref in (send_a, send_b):
            ref[3 + c, 0:16] = both[0]
            ref[3 + c, 16:32] = both[1]
    for c in range(3):
        send_a[c] = ro_ref[c, 3 - 3 * par[0]]
        send_b[c] = ro_ref[c, 3 * par[0]]
    mo_ref[...] = m[3:10]
    cmo_ref[...] = mc[2:13]
    at = lanes((1, 128))
    sum_ref[...] = jnp.where(at == 0, whole, 0.0) + jnp.where(at == 1, part, 0.0)


def third_kernel(
    par, x_ref, r_ref, own, m_ref, cm_ref, xc_ref, rc_ref, a1, b1, a2, b2,
    out_ref, coarse_ref, re, cf, tmp,
):
    for c in range(3):
        re[c, 1:5] = r_ref[c]
        cf[c, 4:6] = own[2 * c : 2 * c + 2]

    def near(up, down):
        for c in range(3):
            re[c, 5] = up[c]
            re[c, 0] = down[c]
            for j in range(2):
                cf[c, 6 + j] = up[3 + c, 16 * j : 16 * j + 16]
                cf[c, 2 + j] = down[3 + c, 16 * j : 16 * j + 16]

    def second(up, down):
        for c in range(3):
            cf[c, 8:10] = up[2 * c : 2 * c + 2]
            cf[c, 0:2] = down[2 * c : 2 * c + 2]

    by_side(par[0], near, a1, b1)
    by_side(par[1], second, a2, b2)

    mc = cm_ref[...]
    pc = inverse(mc, 2)

    def either(shape, a, b):
        return jnp.where(lanes(shape) % 2 == 0, a, b)

    r = [cf[c] for c in range(3)]
    w = [either(r[c].shape, pc[c] * r[c] * FIRST_C, r[c]) for c in range(3)]
    r = [
        jnp.concatenate([r[c][0:4], either((2, 16, 128), r[c][4:6], rc_ref[c]), r[c][6:10]], 0)
        for c in range(3)
    ]
    e = [w[c][3:7] for c in range(3)]
    for k in range(1, 4):
        aw = operate(w, mc[k : 11 - k], 2)
        r = [trim(r[c]) - aw[c] for c in range(3)]
        now, gain = STEPS_C[k - 1]
        if k == 1:
            line = (1, 1, 128)
            now = either(line, now, STEPS_C[6][0])
            gain = either(line, gain, STEPS_C[6][1])
        w = [now * trim(w[c]) + gain * (pc[c][k : 10 - k] * r[c]) for c in range(3)]
        if k == 1:
            col = lax.broadcasted_iota(jnp.int32, (128, 64), 1)
            row = lax.broadcasted_iota(jnp.int32, (128, 64), 0)
            pick = jnp.where(row == 2 * col + 1, 1.0, 0.0).astype(jnp.float32)
            for c in range(3):
                whole = (xc_ref[c] + w[c][3:5]).reshape(32, 128)
                coarse_ref[c] = jnp.dot(
                    whole, pick, precision=lax.Precision.HIGHEST, preferred_element_type=jnp.float32
                ).reshape(2, 16, 64)
        e = [e[c] + w[c][3 - k : 7 - k] for c in range(3)]

    m = m_ref[...]
    order = [0, 0, 1, 1, 2, 2, 3, 3]
    v = [layers(spread(tmp, e[c]), order) for c in range(3)]
    aw = operate(v, m, 1)
    p = inverse(m, 1)
    r = [re[c] - aw[c] for c in range(3)]
    now, gain = STEPS_F[0]
    w = [p[c] * r[c] * FIRST_F for c in range(3)]
    aw = operate(w, m[1:6], 1)
    for c in range(3):
        after = r[c][1:5] - aw[c]
        out_ref[c] = x_ref[c] + v[c][2:6] + (1.0 + now) * w[c][1:5] + gain * (p[c][1:5] * after)


def call(kernel, outs, scratch, par, *args, flops=1 << 22):
    return pl.pallas_call(
        kernel,
        out_shape=[jax.ShapeDtypeStruct(s, jnp.float32) for s in outs],
        in_specs=[pl.BlockSpec(memory_space=pltpu.SMEM)]
        + [pl.BlockSpec(memory_space=pltpu.VMEM)] * len(args),
        out_specs=[pl.BlockSpec(memory_space=pltpu.VMEM)] * len(outs),
        scratch_shapes=[pltpu.VMEM(s, jnp.float32) for s in scratch],
        compiler_params=pltpu.CompilerParams(vmem_limit_bytes=16 << 20),
        cost_estimate=pl.CostEstimate(flops=flops, bytes_accessed=1 << 20, transcendentals=0),
    )(par, *args)


def swap(x, axis, distance, second):
    n = lax.axis_size(axis)
    pairs = []
    for i in range(n - distance):
        if (i // distance) % 2 == second:
            pairs += [(i, i + distance), (i + distance, i)]
    return lax.ppermute(x, axis, pairs)


def body(force, modulus):
    me = lax.axis_index("slab")
    par = jnp.stack([me % 2, (me // 2) % 2, (me // 3) % 2]).astype(jnp.int32)
    odd = me % 2

    def edge(side):
        f = lax.dynamic_slice_in_dim(force, 2 - 2 * side, 2, 1).reshape(6, 32, 128)
        return jnp.concatenate([f, lax.dynamic_slice_in_dim(modulus, 1 - side, 3, 0)], 0)

    a = swap(edge(odd), "slab", 1, 0)
    b = swap(edge(1 - odd), "slab", 1, 1)
    x, big, small = call(
        first_kernel,
        [(3, 4, 32, 128), (22, 32, 128), (9, 16, 128)],
        [(3, 8, 32, 128), (9, 32, 128), (4, 32, 128)],
        par, force, modulus, a, b,
    )
    got = [swap(big, "slab", 1, 0), swap(big, "slab", 1, 1)]
    got += [swap(small, "slab", d, h) for d in (2, 3) for h in (0, 1)]
    x, r, send_a, send_b, small, m, cm, xc, rc, part = call(
        second_kernel,
        [
            (3, 4, 32, 128), (3, 4, 32, 128), (6, 32, 128), (6, 32, 128), (6, 16, 128),
            (7, 32, 128), (11, 16, 128), (3, 2, 16, 128), (3, 2, 16, 128), (1, 128),
        ],
        [(3, 12, 32, 128), (13, 32, 128), (3, 14, 16, 128), (15, 16, 128), (8, 32, 128)],
        par, force, x, big, small, *got,
    )
    n = lax.axis_size("slab")
    got = [swap(send_a, "slab", 1, 0), swap(send_b, "slab", 1, 1)]
    got += [swap(small, "slab", 2, h) for h in (0, 1)]
    sums = lax.all_to_all(jnp.broadcast_to(part[None], (n, 1, 128)), "slab", 0, 0, tiled=True)
    fine, coarse = call(
        third_kernel,
        [(3, 4, 32, 128), (3, 2, 16, 64)],
        [(3, 6, 32, 128), (3, 10, 16, 128), (4, 32, 128)],
        par, x, r, small, m, cm, xc, rc, *got,
    )
    cells = float(modulus.size * n)
    angle = math.acosh(RATIO_C)
    half = math.cosh(CDEG * angle)
    full = math.cosh(2 * CDEG * angle)
    scale = jnp.array([1.0 / cells, 2.0 * half * half / full / 4.0 / (cells / 8.0)], jnp.float32)
    return fine, coarse, sums.sum(axis=(0, 1))[:2] * scale


def solution(mesh):
    return jax.shard_map(
        body,
        mesh=mesh,
        in_specs=(P(None, "slab", None, "sample"), P("slab", None, "sample")),
        out_specs=(P(None, "slab", None, "sample"), P(None, "slab", None, "sample"), P("sample")),
        check_vma=False,
    )
```

```python
import functools
import math

import jax
import jax.numpy as jnp
from jax import lax
from jax.experimental import pallas as pl
from jax.experimental.pallas import tpu as pltpu
from jax.sharding import PartitionSpec as P

SMOOTH = 2
CDEG = 4
FINE = (0.25, 2.0)
COARSE = (0.02, 2.0)


def coefficients(low_end, high_end, degree):
    centre = (high_end + low_end) / 2.0
    half = (high_end - low_end) / 2.0
    ratio = centre / half
    rho = 1.0 / ratio
    steps = []
    for _ in range(degree - 1):
        after = 1.0 / (2.0 * ratio - rho)
        steps.append((after * rho, 2.0 * after / half))
        rho = after
    return 1.0 / centre, steps, ratio


FIRST_F, STEPS_F, _ = coefficients(*FINE, SMOOTH)
FIRST_C, STEPS_C, RATIO_C = coefficients(*COARSE, 2 * CDEG)


def lanes(shape):
    return lax.broadcasted_iota(jnp.int32, shape, len(shape) - 1)


def ahead(v, axis, by=1):
    n = v.shape[axis]
    at = lax.broadcasted_iota(jnp.int32, v.shape, axis)
    return jnp.where(at < n - by, pltpu.roll(v, n - by, axis), 0.0)


def back(v, axis, by=1):
    at = lax.broadcasted_iota(jnp.int32, v.shape, axis)
    return jnp.where(at >= by, pltpu.roll(v, by, axis), 0.0)


def operate(u, m, step):
    low = [c[:-1] for c in u]
    gz = [c[1:] - l for c, l in zip(u, low)]
    gx0 = ahead(low[0], 2, step) - low[0]
    gy1 = ahead(low[1], 1) - low[1]
    s = m * (gx0 + gy1 + gz[2])
    inner = m[1:]
    si = s[1:]
    out = []
    for c in range(3):
        here = low[c][1:]
        fx = inner * (gx0[1:] if c == 0 else ahead(here, 2, step) - here)
        fy = inner * (gy1[1:] if c == 1 else ahead(here, 1) - here)
        fz = m * gz[c]
        if c == 0:
            fx = fx + si
        elif c == 1:
            fy = fy + si
        else:
            fz = fz + s
        out.append((fz[:-1] - fz[1:]) + (back(fy, 1) - fy) + (back(fx, 2, step) - fx))
    return out


def inverse(m, step):
    here = m[1:]
    below = m[:-1]
    by = back(here, 1)
    bx = back(here, 2, step)
    lap = (here + below) + (here + by) + (here + bx) + here
    inside = here > 0.0
    return [
        jnp.where(inside, 1.0 / jnp.where(inside, lap + d, 1.0), 0.0) for d in (bx, by, below)
    ]


def trim(v, n=1):
    return v[n : v.shape[0] - n]


def halve_rows(tmp, v):
    k, rows, _ = v.shape
    tmp[0:k] = v
    return tmp[0:k, pl.ds(0, rows // 2, stride=2), :] + tmp[0:k, pl.ds(1, rows // 2, stride=2), :]


def pack(even_sum, odd_sum):
    even = lanes(even_sum.shape) % 2 == 0
    ax = even_sum.ndim - 1
    near = jnp.where(even, even_sum, odd_sum)
    far = jnp.where(even, pltpu.roll(even_sum, 127, ax), pltpu.roll(odd_sum, 1, ax))
    return near + far


def pair_layers(v):
    return jnp.concatenate([v[i : i + 1] + v[i + 1 : i + 2] for i in range(0, v.shape[0], 2)], 0)


def spread(tmp, e):
    k, rows, _ = e.shape
    even = lanes(e.shape) % 2 == 0
    both = jnp.where(even, e, pltpu.roll(e, 1, 2))
    tmp[0:k, pl.ds(0, rows, stride=2), :] = both
    tmp[0:k, pl.ds(1, rows, stride=2), :] = both
    return tmp[0:k]


def layers(v, order):
    return jnp.concatenate([v[i : i + 1] for i in order], 0)


def by_side(flag, put, a, b):
    lower = flag == 0

    @pl.when(lower)
    def _():
        put(a, b)

    @pl.when(jnp.logical_not(lower))
    def _():
        put(b, a)


def side(ref, c, first, count):
    return ref[c, pl.ds(first, count)]


def first_kernel(
    par, f_ref, e_ref, a_ref, b_ref, s_ref,
    x_ref, r_ref, m_ref, cf_ref, cm_ref, send_a, send_b, far_ref,
    fe, tmp,
):
    for c in range(3):
        fe[c, 4:8] = f_ref[c]
    m_ref[5:9] = 0.4 * e_ref[...]
    m_ref[0:1] = 0.4 * s_ref[...]

    def take(up, down):
        for c in range(3):
            fe[c, 8:12] = up[4 * c : 4 * c + 4]
            fe[c, 0:4] = down[4 * c : 4 * c + 4]
        m_ref[9:13] = 0.4 * up[12:16]
        m_ref[1:5] = 0.4 * down[12:16]

    by_side(par[0], take, a_ref, b_ref)
    m = m_ref[...]
    p = inverse(m, 1)
    r = [fe[c] for c in range(3)]
    w = [p[c] * r[c] * FIRST_F for c in range(3)]
    aw = operate(w, m[1:12], 1)
    r = [trim(r[c]) - aw[c] for c in range(3)]
    now, gain = STEPS_F[0]
    w2 = [now * trim(w[c]) + gain * (trim(p[c]) * r[c]) for c in range(3)]
    aw = operate(w2, m[2:11], 1)
    cm = halve_rows(tmp, pair_layers(m[1:13])) * 0.125
    cm = pack(cm, cm)
    cm_ref[...] = cm
    far_ref[12:18] = cm
    for c in range(3):
        x_ref[c] = w[c][4:8] + w2[c][3:7]
        done = trim(r[c]) - aw[c]
        r_ref[c] = done
        rc = halve_rows(tmp, pair_layers(done)) * 0.5
        fc = halve_rows(tmp, pair_layers(fe[c, 2:10])) * 0.5
        both = pack(rc, fc)
        cf_ref[c] = both
        far_ref[4 * c : 4 * c + 4] = both
    for ref, q in ((send_a, par[0]), (send_b, 1 - par[0])):
        for c in range(3):
            ref[4 * c : 4 * c + 4] = side(r_ref, c, 4 * q, 4)
            for j in range(2):
                ref[14 + c, 16 * j : 16 * j + 16] = cf_ref[c, 2 * q + j]
        ref[12:14] = m_ref[pl.ds(2 + 7 * q, 2)]


def second_kernel(
    top, par, f_ref, x_ref, r_ref, m_ref, own, own_cm, a1, b1, a3, b3,
    xo_ref, ro_ref, far_ref, mo_ref, cmo_ref, coarse_ref, sum_ref,
    re, me, cf, cm, tmp,
):
    for c in range(3):
        re[c, 4:12] = r_ref[c]
        cf[c, 6:10] = own[c]
    me[2:15] = m_ref[...]
    cm[6:12] = own_cm[...]

    def near(up, down):
        for c in range(3):
            re[c, 12:16] = up[4 * c : 4 * c + 4]
            re[c, 0:4] = down[4 * c : 4 * c + 4]
            for j in range(2):
                cf[c, 10 + j] = up[14 + c, 16 * j : 16 * j + 16]
                cf[c, 4 + j] = down[14 + c, 16 * j : 16 * j + 16]
        me[15:17] = up[12:14]
        me[0:2] = down[12:14]

    def third(up, down):
        for c in range(3):
            cf[c, 12:16] = up[4 * c : 4 * c + 4]
            cf[c, 0:4] = down[4 * c : 4 * c + 4]
        cm[12:17] = up[12:17]
        cm[0:6] = down[12:18]

    by_side(par[0], near, a1, b1)
    by_side(par[2], third, a3, b3)

    @pl.when(par[3] == 2)
    def _():
        for c in range(3):
            cf[c, 0:3] = jnp.zeros((3, 16, 128), jnp.float32)
            cf[c, 3] = b3[4 * c + 1]
        cm[0:4] = jnp.zeros((4, 16, 128), jnp.float32)
        cm[4:6] = b3[14:16]

    @pl.when(par[3] == top - 2)
    def _():
        for c in range(3):
            cf[c, 12] = b3[4 * c + 2]
            cf[c, 13:16] = jnp.zeros((3, 16, 128), jnp.float32)
        cm[12:14] = b3[14:16]
        cm[14:17] = jnp.zeros((3, 16, 128), jnp.float32)

    mc = cm[...]
    pc = inverse(mc, 2)
    r = [cf[c] for c in range(3)]
    w = [pc[c] * r[c] * FIRST_C for c in range(3)]
    e = [w[c][3:13] for c in range(3)]
    xc = [w[c][7:9] for c in range(3)]
    part = None
    for k in range(1, 8):
        aw = operate(w, mc[k : 17 - k], 2)
        r = [trim(r[c]) - aw[c] for c in range(3)]
        now, gain = STEPS_C[k - 1]
        if k == 4:
            odd = lanes((2, 16, 128)) % 2 == 1
            part = sum(
                jnp.sum(jnp.where(odd, xc[c] * (cf[c, 7:9] + r[c][3:5]), 0.0)) for c in range(3)
            )
        w = [now * trim(w[c]) + gain * (pc[c][k : 16 - k] * r[c]) for c in range(3)]
        if k <= 3:
            e = [e[c] + w[c][3 - k : 13 - k] for c in range(3)]
        xc = [xc[c] + w[c][7 - k : 9 - k] for c in range(3)]
    col = lax.broadcasted_iota(jnp.int32, (128, 64), 1)
    row = lax.broadcasted_iota(jnp.int32, (128, 64), 0)
    pick = jnp.where(row == 2 * col + 1, 1.0, 0.0).astype(jnp.float32)
    for c in range(3):
        coarse_ref[c] = jnp.dot(
            xc[c].reshape(32, 128), pick,
            precision=lax.Precision.HIGHEST, preferred_element_type=jnp.float32,
        ).reshape(2, 16, 64)

    m = me[...]
    order = [0] + [i for i in range(1, 9) for _ in range(2)] + [9]
    v = [layers(spread(tmp, e[c]), order) for c in range(3)]
    aw = operate(v, m, 1)
    p = inverse(m, 1)
    r = [re[c] - aw[c] for c in range(3)]
    now, gain = STEPS_F[0]
    w = [p[c] * r[c] * FIRST_F for c in range(3)]
    x = [x_ref[c] + v[c][7:11] + w[c][6:10] for c in range(3)]
    aw = operate(w, m[1:16], 1)
    r = [trim(r[c]) - aw[c] for c in range(3)]
    w = [now * trim(w[c]) + gain * (p[c][1:15] * r[c]) for c in range(3)]
    x = [x[c] + w[c][5:9] for c in range(3)]
    aw = operate(w, m[2:15], 1)
    r = [trim(r[c]) - aw[c] for c in range(3)]
    whole = sum(jnp.sum(x[c] * (f_ref[c] + r[c][4:8])) for c in range(3))
    w = [p[c][2:14] * r[c] * FIRST_F for c in range(3)]
    x = [x[c] + w[c][4:8] for c in range(3)]
    aw = operate(w, m[3:14], 1)
    r = [trim(r[c]) - aw[c] for c in range(3)]
    w = [now * trim(w[c]) + gain * (p[c][3:13] * r[c]) for c in range(3)]
    aw = operate(w, m[4:13], 1)
    for c in range(3):
        xo_ref[c] = x[c] + w[c][3:7]
        done = trim(r[c]) - aw[c]
        ro_ref[c] = done[1:7]
        rc = halve_rows(tmp, pair_layers(done)) * 0.5
        far_ref[2 * c : 2 * c + 1] = pack(rc[0:1], rc[1:2])
        far_ref[2 * c + 1 : 2 * c + 2] = pack(rc[2:3], rc[3:4])
    mo_ref[...] = m[5:12]
    cmo_ref[...] = mc[3:14]
    at = lanes((1, 128))
    sum_ref[...] = jnp.where(at == 0, whole, 0.0) + jnp.where(at == 1, part, 0.0)


def third_kernel(top, par, x_ref, r_ref, own, m_ref, cm_ref, a2, b2, out_ref, cf, tmp):
    for c in range(3):
        cf[c, 2:4] = own[2 * c : 2 * c + 2]

    def second(up, down):
        for c in range(3):
            cf[c, 4:6] = up[2 * c : 2 * c + 2]
            cf[c, 0:2] = down[2 * c : 2 * c + 2]

    by_side(par[1], second, a2, b2)
    even = lanes((16, 128)) % 2 == 0

    @pl.when(par[3] == 1)
    def _():
        for c in range(3):
            cf[c, 0] = jnp.zeros((16, 128), jnp.float32)
            cf[c, 1] = jnp.where(even, 0.0, b2[2 * c])

    @pl.when(par[3] == top - 1)
    def _():
        for c in range(3):
            cf[c, 4] = jnp.where(even, b2[2 * c + 1], 0.0)
            cf[c, 5] = jnp.zeros((16, 128), jnp.float32)

    mc = cm_ref[...]
    pc = inverse(mc, 2)
    r = []
    for c in range(3):
        near = cf[c]
        far = pltpu.roll(near, 127, 2)
        parts = [t[i : i + 1] for i in range(6) for t in (near, far)]
        r.append(jnp.concatenate(parts[1:11], 0))
    w = [pc[c] * r[c] * FIRST_C for c in range(3)]
    e = [w[c][3:7] for c in range(3)]
    for k in range(1, 4):
        aw = operate(w, mc[k : 11 - k], 2)
        r = [trim(r[c]) - aw[c] for c in range(3)]
        now, gain = STEPS_C[k - 1]
        w = [now * trim(w[c]) + gain * (pc[c][k : 10 - k] * r[c]) for c in range(3)]
        e = [e[c] + w[c][3 - k : 7 - k] for c in range(3)]

    m = m_ref[...]
    order = [0, 0, 1, 1, 2, 2, 3, 3]
    v = [layers(spread(tmp, e[c]), order) for c in range(3)]
    aw = operate(v, m, 1)
    p = inverse(m, 1)
    r = [r_ref[c] - aw[c] for c in range(3)]
    now, gain = STEPS_F[0]
    w = [p[c] * r[c] * FIRST_F for c in range(3)]
    aw = operate(w, m[1:6], 1)
    for c in range(3):
        after = r[c][1:5] - aw[c]
        out_ref[c] = x_ref[c] + v[c][2:6] + (1.0 + now) * w[c][1:5] + gain * (p[c][1:5] * after)


def call(kernel, outs, scratch, par, *args, flops=1 << 22):
    return pl.pallas_call(
        kernel,
        out_shape=[jax.ShapeDtypeStruct(s, jnp.float32) for s in outs],
        in_specs=[pl.BlockSpec(memory_space=pltpu.SMEM)]
        + [pl.BlockSpec(memory_space=pltpu.VMEM)] * len(args),
        out_specs=[pl.BlockSpec(memory_space=pltpu.VMEM)] * len(outs),
        scratch_shapes=[pltpu.VMEM(s, jnp.float32) for s in scratch],
        compiler_params=pltpu.CompilerParams(vmem_limit_bytes=16 << 20),
        cost_estimate=pl.CostEstimate(flops=flops, bytes_accessed=1 << 20, transcendentals=0),
    )(par, *args)


def half(i, distance):
    return (i // distance + (distance == 3 and i % 3 == 1)) % 2


def swap(x, distance, second, extra=(), axis="slab"):
    n = lax.axis_size(axis)
    pairs = list(extra)
    for i in range(n - distance):
        if half(i, distance) == second:
            pairs += [(i, i + distance), (i + distance, i)]
    return lax.ppermute(x, axis, pairs)


def cycles(force, modulus):
    me = lax.axis_index("slab")
    n = lax.axis_size("slab")
    par = jnp.stack([me % 2, (me // 2) % 2, (me // 3 + (me % 3 == 1)) % 2, me]).astype(jnp.int32)
    top = n - 1
    if half(top, 3) != 1 or half(top - 2, 3) != 1 or half(top, 2) != 1:
        raise ValueError("slab count")
    block = jnp.concatenate([force.reshape(12, 32, 128), modulus], 0)
    a = swap(block, 1, 0)
    b = swap(block, 1, 1)
    s = lax.ppermute(modulus[3:4], "slab", [(i, i + 2) for i in range(n - 2)])
    x, r, m, cf, cm, send_a, send_b, far = call(
        first_kernel,
        [
            (3, 4, 32, 128), (3, 8, 32, 128), (13, 32, 128), (3, 4, 16, 128), (6, 16, 128),
            (17, 32, 128), (17, 32, 128), (18, 16, 128),
        ],
        [(3, 12, 32, 128), (6, 32, 128)],
        par, force, modulus, a, b, s,
    )
    got = [swap(send_a, 1, 0), swap(send_b, 1, 1)]
    got += [swap(far, 3, 0), swap(far, 3, 1, ((0, 2), (top, top - 2)))]
    x, r, far, m, cm, coarse, part = call(
        functools.partial(second_kernel, top),
        [
            (3, 4, 32, 128), (3, 6, 32, 128), (6, 16, 128), (7, 32, 128), (11, 16, 128),
            (3, 2, 16, 64), (1, 128),
        ],
        [(3, 16, 32, 128), (17, 32, 128), (3, 16, 16, 128), (17, 16, 128), (10, 32, 128)],
        par, force, x, r, m, cf, cm, *got,
    )
    got = [swap(far, 2, 0), swap(far, 2, 1, ((0, 1), (top, top - 1)))]
    sums = lax.all_to_all(jnp.broadcast_to(part[None], (n, 1, 128)), "slab", 0, 0, tiled=True)
    (fine,) = call(
        functools.partial(third_kernel, top),
        [(3, 4, 32, 128)],
        [(3, 6, 16, 128), (4, 32, 128)],
        par, x, r, far, m, cm, *got,
    )
    cells = float(modulus.size * n)
    angle = math.acosh(RATIO_C)
    part_way = math.cosh(CDEG * angle)
    full = math.cosh(2 * CDEG * angle)
    scale = jnp.array([1.0 / cells, 2.0 * part_way * part_way / full / 4.0 / (cells / 8.0)], jnp.float32)
    return fine, coarse, sums.sum(axis=(0, 1))[:2] * scale


def solution(mesh):
    return jax.shard_map(
        cycles,
        mesh=mesh,
        in_specs=(P(None, "slab", None, "sample"), P("slab", None, "sample")),
        out_specs=(P(None, "slab", None, "sample"), P(None, "slab", None, "sample"), P("sample")),
        check_vma=False,
    )
```

```python
import functools
import math

import jax
import jax.numpy as jnp
from jax import lax
from jax.experimental import pallas as pl
from jax.experimental.pallas import tpu as pltpu
from jax.sharding import PartitionSpec as P

SMOOTH = 2
CDEG = 4
FINE = (0.25, 2.0)
COARSE = (0.02, 2.0)


def coefficients(low_end, high_end, degree):
    centre = (high_end + low_end) / 2.0
    half = (high_end - low_end) / 2.0
    ratio = centre / half
    rho = 1.0 / ratio
    steps = []
    for _ in range(degree - 1):
        after = 1.0 / (2.0 * ratio - rho)
        steps.append((after * rho, 2.0 * after / half))
        rho = after
    return 1.0 / centre, steps, ratio


FIRST_F, STEPS_F, _ = coefficients(*FINE, SMOOTH)
NOW_F, GAIN_F = STEPS_F[0]
FIRST_C, STEPS_C, RATIO_C = coefficients(*COARSE, 2 * CDEG)


def lanes(shape):
    return lax.broadcasted_iota(jnp.int32, shape, len(shape) - 1)


LINE = (1, 1, 8, 128)


def ahead_x(v, by):
    return jnp.where(lanes(LINE) < 128 - by, pltpu.roll(v, 128 - by, 3), 0.0)


def back_x(v, by):
    return jnp.where(lanes(LINE) >= by, pltpu.roll(v, by, 3), 0.0)


def ahead_y(v):
    at = lax.broadcasted_iota(jnp.int32, LINE, 2)
    moved = jnp.where(at < 7, pltpu.roll(v[:, :1], 7, 2), 0.0)
    return jnp.concatenate([v[:, 1:], moved], 1)


def back_y(v):
    at = lax.broadcasted_iota(jnp.int32, LINE, 2)
    moved = jnp.where(at >= 1, pltpu.roll(v[:, -1:], 1, 2), 0.0)
    return jnp.concatenate([moved, v[:, :-1]], 1)


def operate(u, m, step):
    low = [c[:-1] for c in u]
    gz = [c[1:] - l for c, l in zip(u, low)]
    gx0 = ahead_x(low[0], step) - low[0]
    gy1 = ahead_y(low[1]) - low[1]
    s = m * (gx0 + gy1 + gz[2])
    inner = m[1:]
    si = s[1:]
    out = []
    for c in range(3):
        here = low[c][1:]
        fx = inner * (gx0[1:] if c == 0 else ahead_x(here, step) - here)
        fy = inner * (gy1[1:] if c == 1 else ahead_y(here) - here)
        fz = m * gz[c]
        if c == 0:
            fx = fx + si
        elif c == 1:
            fy = fy + si
        else:
            fz = fz + s
        out.append((fz[:-1] - fz[1:]) + (back_y(fy) - fy) + (back_x(fx, step) - fx))
    return out


def inverse(m, step, scale=1.0):
    here = m[1:]
    below = m[:-1]
    by = back_y(here)
    bx = back_x(here, step)
    lap = (here + below) + (here + by) + (here + bx) + here
    inside = here > 0.0
    return [
        jnp.where(inside, scale / jnp.where(inside, lap + d, 1.0), 0.0) for d in (bx, by, below)
    ]


def trim(v, n=1):
    return v[n : v.shape[0] - n]


def tiles(v):
    return v.reshape(v.shape[0], v.shape[1] // 8, 8, 128)


def rows(v):
    return v.reshape(v.shape[0], v.shape[1] * 8, 128)


def strided(ref, *at):
    return jnp.concatenate([ref[(*at, pl.ds(v, 8, stride=4), slice(None))] for v in range(4)], 0)


def pack(even_sum, odd_sum):
    even = lanes(LINE) % 2 == 0
    near = jnp.where(even, even_sum, odd_sum)
    far = jnp.where(even, pltpu.roll(even_sum, 127, 3), pltpu.roll(odd_sum, 1, 3))
    return near + far


def pair_cells(v):
    out = []
    for i in range(0, v.shape[0], 2):
        t = v[i : i + 1] + v[i + 1 : i + 2]
        out.append(jnp.concatenate([t[:, 0:1] + t[:, 1:2], t[:, 2:3] + t[:, 3:4]], 1))
    return jnp.concatenate(out, 0)


def spread(e, order):
    even = lanes(LINE) % 2 == 0
    both = jnp.where(even, e, pltpu.roll(e, 1, 3))
    wide = jnp.concatenate([both[:, 0:1], both[:, 0:1], both[:, 1:2], both[:, 1:2]], 1)
    return jnp.concatenate([wide[i : i + 1] for i in order], 0)


def by_side(flag, put, a, b):
    lower = flag == 0

    @pl.when(lower)
    def _():
        put(a, b)

    @pl.when(jnp.logical_not(lower))
    def _():
        put(b, a)


def first_kernel(
    par, f_ref, e_ref, a_ref, b_ref, s_ref,
    x_ref, r_ref, m_ref, p_ref, cf_ref, cm_ref, send_a, send_b, far_ref,
    fe,
):
    for z in range(4):
        for c in range(3):
            fe[c, 4 + z] = strided(f_ref, c, z)
        m_ref[5 + z] = 0.4 * strided(e_ref, z)
    m_ref[0] = 0.4 * strided(s_ref, 0)

    def take(up, down):
        for z in range(4):
            for c in range(3):
                fe[c, 8 + z] = strided(up, 4 * c + z)
                fe[c, z] = strided(down, 4 * c + z)
            m_ref[9 + z] = 0.4 * strided(up, 12 + z)
            m_ref[1 + z] = 0.4 * strided(down, 12 + z)

    by_side(par[0], take, a_ref, b_ref)
    m = tiles(m_ref[...])
    p = inverse(m, 1, GAIN_F)
    r = [tiles(fe[c]) for c in range(3)]
    w = [p[c] * r[c] * (FIRST_F / GAIN_F) for c in range(3)]
    aw = operate(w, m[1:12], 1)
    f = r
    r = [trim(r[c]) - aw[c] for c in range(3)]
    w2 = [NOW_F * trim(w[c]) + trim(p[c]) * r[c] for c in range(3)]
    aw = operate(w2, m[2:11], 1)
    cm = pair_cells(m[1:13]) * 0.125
    cm = rows(pack(cm, cm))
    cm_ref[...] = cm
    far_ref[12:18] = cm
    for c in range(3):
        p_ref[c] = rows(p[c])
        x_ref[c] = rows(w[c][4:8] + w2[c][3:7])
        done = trim(r[c]) - aw[c]
        r_ref[c] = rows(done)
        both = rows(pack(pair_cells(done) * 0.5, pair_cells(f[c][2:10]) * 0.5))
        cf_ref[c] = both
        far_ref[4 * c : 4 * c + 4] = both
    for ref, q in ((send_a, par[0]), (send_b, 1 - par[0])):
        for c in range(3):
            ref[4 * c : 4 * c + 4] = r_ref[c, pl.ds(4 * q, 4)]
            for j in range(2):
                ref[14 + c, 16 * j : 16 * j + 16] = cf_ref[c, 2 * q + j]
        ref[12:14] = m_ref[pl.ds(2 + 7 * q, 2)]


def second_kernel(
    top, par, f_ref, x_ref, r_ref, m_ref, p_ref, own, own_cm, a1, b1, a3, b3,
    xo_ref, ro_ref, far_ref, cmo_ref, pco_ref, xc_ref, rc_ref, wc_ref, sum_ref,
    re, me, cf, cm,
):
    for c in range(3):
        re[c, 4:12] = r_ref[c]
        cf[c, 6:10] = own[c]
    me[2:15] = m_ref[...]
    cm[6:12] = own_cm[...]

    def near(up, down):
        for c in range(3):
            re[c, 12:16] = up[4 * c : 4 * c + 4]
            re[c, 0:4] = down[4 * c : 4 * c + 4]
            for j in range(2):
                cf[c, 10 + j] = up[14 + c, 16 * j : 16 * j + 16]
                cf[c, 4 + j] = down[14 + c, 16 * j : 16 * j + 16]
        me[15:17] = up[12:14]
        me[0:2] = down[12:14]

    def third(up, down):
        for c in range(3):
            cf[c, 12:16] = up[4 * c : 4 * c + 4]
            cf[c, 0:4] = down[4 * c : 4 * c + 4]
        cm[12:17] = up[12:17]
        cm[0:6] = down[12:18]

    by_side(par[0], near, a1, b1)
    by_side(par[2], third, a3, b3)

    @pl.when(par[3] == 2)
    def _():
        for c in range(3):
            cf[c, 0:3] = jnp.zeros((3, 16, 128), jnp.float32)
            cf[c, 3] = b3[4 * c + 1]
        cm[0:4] = jnp.zeros((4, 16, 128), jnp.float32)
        cm[4:6] = b3[14:16]

    @pl.when(par[3] == top - 2)
    def _():
        for c in range(3):
            cf[c, 12] = b3[4 * c + 2]
            cf[c, 13:16] = jnp.zeros((3, 16, 128), jnp.float32)
        cm[12:14] = b3[14:16]
        cm[14:17] = jnp.zeros((3, 16, 128), jnp.float32)

    mc = tiles(cm[...])
    pc = inverse(mc, 2)
    r = [tiles(cf[c]) for c in range(3)]
    own_rhs = [t[7:9] for t in r]
    w = [pc[c] * r[c] * FIRST_C for c in range(3)]
    e = [w[c][3:13] for c in range(3)]
    xc = [w[c][7:9] for c in range(3)]
    part = None
    for k in range(1, 5):
        aw = operate(w, mc[k : 17 - k], 2)
        r = [trim(r[c]) - aw[c] for c in range(3)]
        now, gain = STEPS_C[k - 1]
        if k == 4:
            odd = lanes(LINE) % 2 == 1
            part = sum(
                jnp.sum(jnp.where(odd, xc[c] * (own_rhs[c] + r[c][3:5]), 0.0)) for c in range(3)
            )
        w = [now * trim(w[c]) + gain * (pc[c][k : 16 - k] * r[c]) for c in range(3)]
        if k <= 3:
            e = [e[c] + w[c][3 - k : 13 - k] for c in range(3)]
        xc = [xc[c] + w[c][7 - k : 9 - k] for c in range(3)]
    for c in range(3):
        xc_ref[c] = rows(xc[c])
        rc_ref[c] = rows(r[c])
        wc_ref[c] = rows(w[c])
        pco_ref[c] = rows(pc[c][3:13])

    m = tiles(me[...])
    order = [0] + [i for i in range(1, 9) for _ in range(2)] + [9]
    v = [spread(e[c], order) for c in range(3)]
    aw = operate(v, m, 1)
    low = inverse(m[0:3], 1, GAIN_F)
    high = inverse(m[14:17], 1, GAIN_F)
    p = [jnp.concatenate([low[c], tiles(p_ref[c]), high[c]], 0) for c in range(3)]
    r = [tiles(re[c]) - aw[c] for c in range(3)]
    start = FIRST_F / GAIN_F
    w = [p[c] * r[c] * start for c in range(3)]
    x = [tiles(x_ref[c]) + v[c][7:11] + w[c][6:10] for c in range(3)]
    aw = operate(w, m[1:16], 1)
    r = [trim(r[c]) - aw[c] for c in range(3)]
    w = [NOW_F * trim(w[c]) + p[c][1:15] * r[c] for c in range(3)]
    x = [x[c] + w[c][5:9] for c in range(3)]
    aw = operate(w, m[2:15], 1)
    r = [trim(r[c]) - aw[c] for c in range(3)]
    f = [
        jnp.concatenate([strided(f_ref, c, z).reshape(1, 4, 8, 128) for z in range(4)], 0)
        for c in range(3)
    ]
    whole = sum(jnp.sum(x[c] * (f[c] + r[c][4:8])) for c in range(3))
    w = [p[c][2:14] * r[c] * start for c in range(3)]
    x = [x[c] + w[c][4:8] for c in range(3)]
    aw = operate(w, m[3:14], 1)
    r = [trim(r[c]) - aw[c] for c in range(3)]
    w = [NOW_F * trim(w[c]) + p[c][3:13] * r[c] for c in range(3)]
    aw = operate(w, m[4:13], 1)
    for c in range(3):
        xo_ref[c] = rows(x[c] + w[c][3:7])
        done = trim(r[c]) - aw[c]
        ro_ref[c] = rows(done[1:7])
        rc = pair_cells(done) * 0.5
        far_ref[2 * c : 2 * c + 1] = rows(pack(rc[0:1], rc[1:2]))
        far_ref[2 * c + 1 : 2 * c + 2] = rows(pack(rc[2:3], rc[3:4]))
    cmo_ref[...] = cm[3:14]
    at = lanes((1, 128))
    line = jnp.where(at == 0, whole, 0.0) + jnp.where(at == 1, part, 0.0)
    sum_ref[...] = jnp.broadcast_to(line[None], sum_ref.shape)


def late_kernel(cm_ref, pc_ref, xc_ref, rc_ref, wc_ref, coarse_ref):
    mc = tiles(cm_ref[...])
    pc = [tiles(pc_ref[c]) for c in range(3)]
    xc = [tiles(xc_ref[c]) for c in range(3)]
    r = [tiles(rc_ref[c]) for c in range(3)]
    w = [tiles(wc_ref[c]) for c in range(3)]
    for k in range(5, 8):
        aw = operate(w, mc[k - 3 : 14 - k], 2)
        r = [trim(r[c]) - aw[c] for c in range(3)]
        now, gain = STEPS_C[k - 1]
        w = [now * trim(w[c]) + gain * (pc[c][k - 3 : 13 - k] * r[c]) for c in range(3)]
        xc = [xc[c] + w[c][7 - k : 9 - k] for c in range(3)]
    col = lax.broadcasted_iota(jnp.int32, (128, 64), 1)
    row = lax.broadcasted_iota(jnp.int32, (128, 64), 0)
    pick = jnp.where(row == 2 * col + 1, 1.0, 0.0).astype(jnp.float32)
    for c in range(3):
        solved = jnp.dot(
            xc[c].reshape(32, 128), pick,
            precision=lax.Precision.HIGHEST, preferred_element_type=jnp.float32,
        )
        for z in range(2):
            for t in range(2):
                at = 16 * z + 8 * t
                coarse_ref[c, z, pl.ds(t, 8, stride=2), :] = solved[at : at + 8]


def third_kernel(
    top, scale, par, x_ref, r_ref, own, m_ref, p_ref, cm_ref, pc_ref, sums, a2, b2, out_ref, sum_ref, cf
):
    for c in range(3):
        cf[c, 2:4] = own[2 * c : 2 * c + 2]

    def second(up, down):
        for c in range(3):
            cf[c, 4:6] = up[2 * c : 2 * c + 2]
            cf[c, 0:2] = down[2 * c : 2 * c + 2]

    by_side(par[1], second, a2, b2)
    even = lanes((16, 128)) % 2 == 0

    @pl.when(par[3] == 1)
    def _():
        for c in range(3):
            cf[c, 0] = jnp.zeros((16, 128), jnp.float32)
            cf[c, 1] = jnp.where(even, 0.0, b2[2 * c])

    @pl.when(par[3] == top - 1)
    def _():
        for c in range(3):
            cf[c, 4] = jnp.where(even, b2[2 * c + 1], 0.0)
            cf[c, 5] = jnp.zeros((16, 128), jnp.float32)

    for k in range(2):
        sum_ref[k] = jnp.sum(jnp.where(lanes((64, 1, 128)) == k, sums[...], 0.0)) * scale[k]
    mc = tiles(cm_ref[...])
    pc = [tiles(pc_ref[c]) for c in range(3)]
    r = []
    for c in range(3):
        near = tiles(cf[c])
        far = pltpu.roll(near, 127, 3)
        parts = [t[i : i + 1] for i in range(6) for t in (near, far)]
        r.append(jnp.concatenate(parts[1:11], 0))
    w = [pc[c] * r[c] * FIRST_C for c in range(3)]
    e = [w[c][3:7] for c in range(3)]
    for k in range(1, 4):
        aw = operate(w, mc[k : 11 - k], 2)
        r = [trim(r[c]) - aw[c] for c in range(3)]
        now, gain = STEPS_C[k - 1]
        w = [now * trim(w[c]) + gain * (pc[c][k : 10 - k] * r[c]) for c in range(3)]
        e = [e[c] + w[c][3 - k : 7 - k] for c in range(3)]

    m = tiles(m_ref[3:10])
    order = [0, 0, 1, 1, 2, 2, 3, 3]
    v = [spread(e[c], order) for c in range(3)]
    aw = operate(v, m, 1)
    p = [tiles(p_ref[c, 3:9]) for c in range(3)]
    r = [tiles(r_ref[c]) - aw[c] for c in range(3)]
    w = [p[c] * r[c] * (FIRST_F / GAIN_F) for c in range(3)]
    aw = operate(w, m[1:6], 1)
    for c in range(3):
        after = r[c][1:5] - aw[c]
        x = tiles(x_ref[c]) + v[c][2:6] + (1.0 + NOW_F) * w[c][1:5] + p[c][1:5] * after
        for z in range(4):
            for t in range(4):
                out_ref[c, z, pl.ds(t, 8, stride=4), :] = x[z, t]


def call(kernel, outs, scratch, *args, par=None, small=(), flops=1 << 22):
    head = () if par is None else (par,)
    places = [pltpu.SMEM if i in small else pltpu.VMEM for i in range(len(outs))]
    return pl.pallas_call(
        kernel,
        out_shape=[jax.ShapeDtypeStruct(s, jnp.float32) for s in outs],
        in_specs=[pl.BlockSpec(memory_space=pltpu.SMEM)] * len(head)
        + [pl.BlockSpec(memory_space=pltpu.VMEM)] * len(args),
        out_specs=[pl.BlockSpec(memory_space=place) for place in places],
        scratch_shapes=[pltpu.VMEM(s, jnp.float32) for s in scratch],
        compiler_params=pltpu.CompilerParams(vmem_limit_bytes=16 << 20),
        cost_estimate=pl.CostEstimate(flops=flops, bytes_accessed=1 << 20, transcendentals=0),
    )(*head, *args)


def half(i, distance):
    return (i // distance + (distance == 3 and i % 3 == 1)) % 2


def swap(x, distance, second, extra=(), axis="slab"):
    n = lax.axis_size(axis)
    pairs = list(extra)
    for i in range(n - distance):
        if half(i, distance) == second:
            pairs += [(i, i + distance), (i + distance, i)]
    return lax.ppermute(x, axis, pairs)


def cycles(force, modulus):
    me = lax.axis_index("slab")
    n = lax.axis_size("slab")
    par = jnp.stack([me % 2, (me // 2) % 2, (me // 3 + (me % 3 == 1)) % 2, me]).astype(jnp.int32)
    top = n - 1
    if half(top, 3) != 1 or half(top - 2, 3) != 1 or half(top, 2) != 1:
        raise ValueError("slab count")
    block = jnp.concatenate([force.reshape(12, 32, 128), modulus], 0)
    a = swap(block, 1, 0)
    b = swap(block, 1, 1)
    s = lax.ppermute(modulus[3:4], "slab", [(i, i + 2) for i in range(n - 2)])
    x, r, m, p, cf, cm, send_a, send_b, far = call(
        first_kernel,
        [
            (3, 4, 32, 128), (3, 8, 32, 128), (13, 32, 128), (3, 12, 32, 128), (3, 4, 16, 128),
            (6, 16, 128), (17, 32, 128), (17, 32, 128), (18, 16, 128),
        ],
        [(3, 12, 32, 128)],
        force, modulus, a, b, s, par=par,
    )
    got = [swap(send_a, 1, 0), swap(send_b, 1, 1)]
    got += [swap(far, 3, 0), swap(far, 3, 1, ((0, 2), (top, top - 2)))]
    x, r, far, cm, pc, xc, rc, wc, part = call(
        functools.partial(second_kernel, top),
        [
            (3, 4, 32, 128), (3, 6, 32, 128), (6, 16, 128), (11, 16, 128), (3, 10, 16, 128),
            (3, 2, 16, 128), (3, 8, 16, 128), (3, 8, 16, 128), (n, 1, 128),
        ],
        [(3, 16, 32, 128), (17, 32, 128), (3, 16, 16, 128), (17, 16, 128)],
        force, x, r, m, p, cf, cm, *got, par=par,
    )
    got = [swap(far, 2, 0), swap(far, 2, 1, ((0, 1), (top, top - 1)))]
    sums = lax.all_to_all(part, "slab", 0, 0, tiled=True)
    (coarse,) = call(late_kernel, [(3, 2, 16, 64)], [], cm, pc, xc, rc, wc)
    cells = float(modulus.size * n)
    angle = math.acosh(RATIO_C)
    part_way = math.cosh(CDEG * angle)
    full = math.cosh(2 * CDEG * angle)
    scale = (1.0 / cells, 2.0 * part_way * part_way / full / 4.0 / (cells / 8.0))
    fine, total = call(
        functools.partial(third_kernel, top, scale),
        [(3, 4, 32, 128), (2,)],
        [(3, 6, 16, 128)],
        x, r, far, m, p, cm, pc, sums, *got, par=par, small=(1,),
    )
    return fine, coarse, total


def solution(mesh):
    return jax.shard_map(
        cycles,
        mesh=mesh,
        in_specs=(P(None, "slab", None, "sample"), P("slab", None, "sample")),
        out_specs=(P(None, "slab", None, "sample"), P(None, "slab", None, "sample"), P("sample")),
        check_vma=False,
    )
```

```python
import functools
import math

import jax
import jax.numpy as jnp
from jax import lax
from jax.experimental import pallas as pl
from jax.experimental.pallas import tpu as pltpu
from jax.sharding import PartitionSpec as P

SMOOTH = 2
CDEG = 4
FINE = (0.25, 2.0)
COARSE = (0.02, 2.0)


def coefficients(low_end, high_end, degree):
    centre = (high_end + low_end) / 2.0
    half = (high_end - low_end) / 2.0
    ratio = centre / half
    rho = 1.0 / ratio
    steps = []
    for _ in range(degree - 1):
        after = 1.0 / (2.0 * ratio - rho)
        steps.append((after * rho, 2.0 * after / half))
        rho = after
    return 1.0 / centre, steps, ratio


FIRST_F, STEPS_F, _ = coefficients(*FINE, SMOOTH)
NOW_F, GAIN_F = STEPS_F[0]
FIRST_C, STEPS_C, RATIO_C = coefficients(*COARSE, 2 * CDEG)


def lanes(shape):
    return lax.broadcasted_iota(jnp.int32, shape, len(shape) - 1)


LINE = (1, 1, 8, 128)


def ahead_x(v, by):
    return jnp.where(lanes(LINE) < 128 - by, pltpu.roll(v, 128 - by, 3), 0.0)


def back_x(v, by):
    return jnp.where(lanes(LINE) >= by, pltpu.roll(v, by, 3), 0.0)


def ahead_y(v):
    at = lax.broadcasted_iota(jnp.int32, LINE, 2)
    moved = jnp.where(at < 7, pltpu.roll(v[:, :1], 7, 2), 0.0)
    return jnp.concatenate([v[:, 1:], moved], 1)


def back_y(v):
    at = lax.broadcasted_iota(jnp.int32, LINE, 2)
    moved = jnp.where(at >= 1, pltpu.roll(v[:, -1:], 1, 2), 0.0)
    return jnp.concatenate([moved, v[:, :-1]], 1)


def operate(u, m, step):
    low = [c[:-1] for c in u]
    gz = [c[1:] - l for c, l in zip(u, low)]
    gx0 = ahead_x(low[0], step) - low[0]
    gy1 = ahead_y(low[1]) - low[1]
    s = m * (gx0 + gy1 + gz[2])
    inner = m[1:]
    si = s[1:]
    out = []
    for c in range(3):
        here = low[c][1:]
        fx = inner * (gx0[1:] if c == 0 else ahead_x(here, step) - here)
        fy = inner * (gy1[1:] if c == 1 else ahead_y(here) - here)
        fz = m * gz[c]
        if c == 0:
            fx = fx + si
        elif c == 1:
            fy = fy + si
        else:
            fz = fz + s
        out.append((fz[:-1] - fz[1:]) + (back_y(fy) - fy) + (back_x(fx, step) - fx))
    return out


def inverse(m, step, scale=1.0):
    here = m[1:]
    below = m[:-1]
    by = back_y(here)
    bx = back_x(here, step)
    lap = (here + below) + (here + by) + (here + bx) + here
    inside = here > 0.0
    return [
        jnp.where(inside, scale / jnp.where(inside, lap + d, 1.0), 0.0) for d in (bx, by, below)
    ]


def trim(v, n=1):
    return v[n : v.shape[0] - n]


def tiles(v):
    return v.reshape(v.shape[0], v.shape[1] // 8, 8, 128)


def rows(v):
    return v.reshape(v.shape[0], v.shape[1] * 8, 128)


def strided(ref, *at):
    return jnp.concatenate([ref[(*at, pl.ds(v, 8, stride=4), slice(None))] for v in range(4)], 0)


def pack(even_sum, odd_sum):
    even = lanes(LINE) % 2 == 0
    near = jnp.where(even, even_sum, odd_sum)
    far = jnp.where(even, pltpu.roll(even_sum, 127, 3), pltpu.roll(odd_sum, 1, 3))
    return near + far


def pair_cells(v):
    out = []
    for i in range(0, v.shape[0], 2):
        t = v[i : i + 1] + v[i + 1 : i + 2]
        out.append(jnp.concatenate([t[:, 0:1] + t[:, 1:2], t[:, 2:3] + t[:, 3:4]], 1))
    return jnp.concatenate(out, 0)


def spread(e, order):
    even = lanes(LINE) % 2 == 0
    both = jnp.where(even, e, pltpu.roll(e, 1, 3))
    wide = jnp.concatenate([both[:, 0:1], both[:, 0:1], both[:, 1:2], both[:, 1:2]], 1)
    return jnp.concatenate([wide[i : i + 1] for i in order], 0)


def by_side(flag, put, a, b):
    lower = flag == 0

    @pl.when(lower)
    def _():
        put(a, b)

    @pl.when(jnp.logical_not(lower))
    def _():
        put(b, a)


def first_kernel(
    f_ref, e_ref, a_ref, b_ref, s_ref,
    x_ref, r_ref, m_ref, p_ref, cf_ref, cm_ref, send_a, send_b, far_ref,
    fe,
):
    for z in range(4):
        for c in range(3):
            fe[c, 4 + z] = strided(f_ref, c, z)
        m_ref[5 + z] = 0.4 * strided(e_ref, z)
    m_ref[0] = 0.4 * strided(s_ref, 0)

    def take(up, down):
        for z in range(4):
            for c in range(3):
                fe[c, 8 + z] = strided(up, 4 * c + z)
                fe[c, z] = strided(down, 4 * c + z)
            m_ref[9 + z] = 0.4 * strided(up, 12 + z)
            m_ref[1 + z] = 0.4 * strided(down, 12 + z)

    me = lax.axis_index("slab")
    by_side(me % 2, take, a_ref, b_ref)
    m = tiles(m_ref[...])
    p = inverse(m, 1, GAIN_F)
    r = [tiles(fe[c]) for c in range(3)]
    w = [p[c] * r[c] * (FIRST_F / GAIN_F) for c in range(3)]
    aw = operate(w, m[1:12], 1)
    f = r
    r = [trim(r[c]) - aw[c] for c in range(3)]
    w2 = [NOW_F * trim(w[c]) + trim(p[c]) * r[c] for c in range(3)]
    aw = operate(w2, m[2:11], 1)
    cm = pair_cells(m[1:13]) * 0.125
    cm = rows(pack(cm, cm))
    cm_ref[...] = cm
    far_ref[12:18] = cm
    for c in range(3):
        p_ref[c] = rows(p[c])
        x_ref[c] = rows(w[c][4:8] + w2[c][3:7])
        done = trim(r[c]) - aw[c]
        r_ref[c] = rows(done)
        both = rows(pack(pair_cells(done) * 0.5, pair_cells(f[c][2:10]) * 0.5))
        cf_ref[c] = both
        far_ref[4 * c : 4 * c + 4] = both
    for ref, q in ((send_a, me % 2), (send_b, 1 - me % 2)):
        for c in range(3):
            ref[4 * c : 4 * c + 4] = r_ref[c, pl.ds(4 * q, 4)]
            for j in range(2):
                ref[14 + c, 16 * j : 16 * j + 16] = cf_ref[c, 2 * q + j]
        ref[12:14] = m_ref[pl.ds(2 + 7 * q, 2)]


def second_kernel(
    top, f_ref, x_ref, r_ref, m_ref, p_ref, own, own_cm, a1, b1, a3, b3,
    xo_ref, ro_ref, far_ref, cmo_ref, pco_ref, xc_ref, rc_ref, wc_ref, sum_ref,
    re, me, cf, cm,
):
    for c in range(3):
        re[c, 4:12] = r_ref[c]
        cf[c, 6:10] = own[c]
    me[2:15] = m_ref[...]
    cm[6:12] = own_cm[...]

    def near(up, down):
        for c in range(3):
            re[c, 12:16] = up[4 * c : 4 * c + 4]
            re[c, 0:4] = down[4 * c : 4 * c + 4]
            for j in range(2):
                cf[c, 10 + j] = up[14 + c, 16 * j : 16 * j + 16]
                cf[c, 4 + j] = down[14 + c, 16 * j : 16 * j + 16]
        me[15:17] = up[12:14]
        me[0:2] = down[12:14]

    def third(up, down):
        for c in range(3):
            cf[c, 12:16] = up[4 * c : 4 * c + 4]
            cf[c, 0:4] = down[4 * c : 4 * c + 4]
        cm[12:17] = up[12:17]
        cm[0:6] = down[12:18]

    place = lax.axis_index("slab")
    by_side(half(place, 1), near, a1, b1)
    by_side(half(place, 3), third, a3, b3)

    @pl.when(place == 2)
    def _():
        for c in range(3):
            cf[c, 0:3] = jnp.zeros((3, 16, 128), jnp.float32)
            cf[c, 3] = b3[4 * c + 1]
        cm[0:4] = jnp.zeros((4, 16, 128), jnp.float32)
        cm[4:6] = b3[14:16]

    @pl.when(place == top - 2)
    def _():
        for c in range(3):
            cf[c, 12] = b3[4 * c + 2]
            cf[c, 13:16] = jnp.zeros((3, 16, 128), jnp.float32)
        cm[12:14] = b3[14:16]
        cm[14:17] = jnp.zeros((3, 16, 128), jnp.float32)

    mc = tiles(cm[...])
    pc = inverse(mc, 2)
    r = [tiles(cf[c]) for c in range(3)]
    own_rhs = [t[7:9] for t in r]
    w = [pc[c] * r[c] * FIRST_C for c in range(3)]
    e = [w[c][3:13] for c in range(3)]
    xc = [w[c][7:9] for c in range(3)]
    part = None
    for k in range(1, 5):
        aw = operate(w, mc[k : 17 - k], 2)
        r = [trim(r[c]) - aw[c] for c in range(3)]
        now, gain = STEPS_C[k - 1]
        if k == 4:
            odd = lanes(LINE) % 2 == 1
            part = sum(
                jnp.sum(jnp.where(odd, xc[c] * (own_rhs[c] + r[c][3:5]), 0.0)) for c in range(3)
            )
        w = [now * trim(w[c]) + gain * (pc[c][k : 16 - k] * r[c]) for c in range(3)]
        if k <= 3:
            e = [e[c] + w[c][3 - k : 13 - k] for c in range(3)]
        xc = [xc[c] + w[c][7 - k : 9 - k] for c in range(3)]
    for c in range(3):
        xc_ref[c] = rows(xc[c])
        rc_ref[c] = rows(r[c])
        wc_ref[c] = rows(w[c])
        pco_ref[c] = rows(pc[c][3:13])

    m = tiles(me[...])
    order = [0] + [i for i in range(1, 9) for _ in range(2)] + [9]
    v = [spread(e[c], order) for c in range(3)]
    aw = operate(v, m, 1)
    low = inverse(m[0:3], 1, GAIN_F)
    high = inverse(m[14:17], 1, GAIN_F)
    p = [jnp.concatenate([low[c], tiles(p_ref[c]), high[c]], 0) for c in range(3)]
    r = [tiles(re[c]) - aw[c] for c in range(3)]
    start = FIRST_F / GAIN_F
    w = [p[c] * r[c] * start for c in range(3)]
    x = [tiles(x_ref[c]) + v[c][7:11] + w[c][6:10] for c in range(3)]
    aw = operate(w, m[1:16], 1)
    r = [trim(r[c]) - aw[c] for c in range(3)]
    w = [NOW_F * trim(w[c]) + p[c][1:15] * r[c] for c in range(3)]
    x = [x[c] + w[c][5:9] for c in range(3)]
    aw = operate(w, m[2:15], 1)
    r = [trim(r[c]) - aw[c] for c in range(3)]
    f = [
        jnp.concatenate([strided(f_ref, c, z).reshape(1, 4, 8, 128) for z in range(4)], 0)
        for c in range(3)
    ]
    whole = sum(jnp.sum(x[c] * (f[c] + r[c][4:8])) for c in range(3))
    w = [p[c][2:14] * r[c] * start for c in range(3)]
    x = [x[c] + w[c][4:8] for c in range(3)]
    aw = operate(w, m[3:14], 1)
    r = [trim(r[c]) - aw[c] for c in range(3)]
    w = [NOW_F * trim(w[c]) + p[c][3:13] * r[c] for c in range(3)]
    aw = operate(w, m[4:13], 1)
    for c in range(3):
        xo_ref[c] = rows(x[c] + w[c][3:7])
        done = trim(r[c]) - aw[c]
        ro_ref[c] = rows(done[1:7])
        rc = pair_cells(done) * 0.5
        far_ref[2 * c : 2 * c + 1] = rows(pack(rc[0:1], rc[1:2]))
        far_ref[2 * c + 1 : 2 * c + 2] = rows(pack(rc[2:3], rc[3:4]))
    cmo_ref[...] = cm[3:14]
    at = lanes((1, 128))
    line = jnp.where(at == 0, whole, 0.0) + jnp.where(at == 1, part, 0.0)
    sum_ref[...] = jnp.broadcast_to(line[None], sum_ref.shape)


def late_kernel(cm_ref, pc_ref, xc_ref, rc_ref, wc_ref, coarse_ref):
    mc = tiles(cm_ref[...])
    pc = [tiles(pc_ref[c]) for c in range(3)]
    xc = [tiles(xc_ref[c]) for c in range(3)]
    r = [tiles(rc_ref[c]) for c in range(3)]
    w = [tiles(wc_ref[c]) for c in range(3)]
    for k in range(5, 8):
        aw = operate(w, mc[k - 3 : 14 - k], 2)
        r = [trim(r[c]) - aw[c] for c in range(3)]
        now, gain = STEPS_C[k - 1]
        w = [now * trim(w[c]) + gain * (pc[c][k - 3 : 13 - k] * r[c]) for c in range(3)]
        xc = [xc[c] + w[c][7 - k : 9 - k] for c in range(3)]
    col = lax.broadcasted_iota(jnp.int32, (128, 64), 1)
    row = lax.broadcasted_iota(jnp.int32, (128, 64), 0)
    pick = jnp.where(row == 2 * col + 1, 1.0, 0.0).astype(jnp.float32)
    for c in range(3):
        solved = jnp.dot(
            xc[c].reshape(32, 128), pick,
            precision=lax.Precision.HIGHEST, preferred_element_type=jnp.float32,
        )
        for z in range(2):
            for t in range(2):
                at = 16 * z + 8 * t
                coarse_ref[c, z, pl.ds(t, 8, stride=2), :] = solved[at : at + 8]


def third_kernel(
    top, scale, x_ref, r_ref, own, m_ref, p_ref, cm_ref, pc_ref, sums, a2, b2, out_ref, sum_ref, cf
):
    for c in range(3):
        cf[c, 2:4] = own[2 * c : 2 * c + 2]

    def second(up, down):
        for c in range(3):
            cf[c, 4:6] = up[2 * c : 2 * c + 2]
            cf[c, 0:2] = down[2 * c : 2 * c + 2]

    place = lax.axis_index("slab")
    by_side(half(place, 2), second, a2, b2)
    even = lanes((16, 128)) % 2 == 0

    @pl.when(place == 1)
    def _():
        for c in range(3):
            cf[c, 0] = jnp.zeros((16, 128), jnp.float32)
            cf[c, 1] = jnp.where(even, 0.0, b2[2 * c])

    @pl.when(place == top - 1)
    def _():
        for c in range(3):
            cf[c, 4] = jnp.where(even, b2[2 * c + 1], 0.0)
            cf[c, 5] = jnp.zeros((16, 128), jnp.float32)

    for k in range(2):
        sum_ref[k] = jnp.sum(jnp.where(lanes((64, 1, 128)) == k, sums[...], 0.0)) * scale[k]
    mc = tiles(cm_ref[...])
    pc = [tiles(pc_ref[c]) for c in range(3)]
    r = []
    for c in range(3):
        near = tiles(cf[c])
        far = pltpu.roll(near, 127, 3)
        parts = [t[i : i + 1] for i in range(6) for t in (near, far)]
        r.append(jnp.concatenate(parts[1:11], 0))
    w = [pc[c] * r[c] * FIRST_C for c in range(3)]
    e = [w[c][3:7] for c in range(3)]
    for k in range(1, 4):
        aw = operate(w, mc[k : 11 - k], 2)
        r = [trim(r[c]) - aw[c] for c in range(3)]
        now, gain = STEPS_C[k - 1]
        w = [now * trim(w[c]) + gain * (pc[c][k : 10 - k] * r[c]) for c in range(3)]
        e = [e[c] + w[c][3 - k : 7 - k] for c in range(3)]

    m = tiles(m_ref[3:10])
    order = [0, 0, 1, 1, 2, 2, 3, 3]
    v = [spread(e[c], order) for c in range(3)]
    aw = operate(v, m, 1)
    p = [tiles(p_ref[c, 3:9]) for c in range(3)]
    r = [tiles(r_ref[c]) - aw[c] for c in range(3)]
    w = [p[c] * r[c] * (FIRST_F / GAIN_F) for c in range(3)]
    aw = operate(w, m[1:6], 1)
    for c in range(3):
        after = r[c][1:5] - aw[c]
        x = tiles(x_ref[c]) + v[c][2:6] + (1.0 + NOW_F) * w[c][1:5] + p[c][1:5] * after
        for z in range(4):
            for t in range(4):
                out_ref[c, z, pl.ds(t, 8, stride=4), :] = x[z, t]


def call(kernel, outs, scratch, *args, small=(), flops=1 << 22):
    places = [pltpu.SMEM if i in small else pltpu.VMEM for i in range(len(outs))]
    return pl.pallas_call(
        kernel,
        out_shape=[jax.ShapeDtypeStruct(s, jnp.float32) for s in outs],
        in_specs=[pl.BlockSpec(memory_space=pltpu.VMEM)] * len(args),
        out_specs=[pl.BlockSpec(memory_space=place) for place in places],
        scratch_shapes=[pltpu.VMEM(s, jnp.float32) for s in scratch],
        compiler_params=pltpu.CompilerParams(vmem_limit_bytes=16 << 20),
        cost_estimate=pl.CostEstimate(flops=flops, bytes_accessed=1 << 20, transcendentals=0),
    )(*args)


def half(i, distance):
    if distance == 3:
        i = i + 3 * (i % 3) * (2 - i % 3)
    return (i // distance) % 2


def swap(x, distance, second, extra=(), axis="slab"):
    n = lax.axis_size(axis)
    pairs = list(extra)
    for i in range(n - distance):
        if half(i, distance) == second:
            pairs += [(i, i + distance), (i + distance, i)]
    return lax.ppermute(x, axis, pairs)


def cycles(force, modulus):
    n = lax.axis_size("slab")
    top = n - 1
    if half(top, 3) != 1 or half(top - 2, 3) != 1 or half(top, 2) != 1:
        raise ValueError("slab count")
    block = jnp.concatenate([force.reshape(12, 32, 128), modulus], 0)
    a = swap(block, 1, 0)
    b = swap(block, 1, 1)
    s = lax.ppermute(modulus[3:4], "slab", [(i, i + 2) for i in range(n - 2)])
    x, r, m, p, cf, cm, send_a, send_b, far = call(
        first_kernel,
        [
            (3, 4, 32, 128), (3, 8, 32, 128), (13, 32, 128), (3, 12, 32, 128), (3, 4, 16, 128),
            (6, 16, 128), (17, 32, 128), (17, 32, 128), (18, 16, 128),
        ],
        [(3, 12, 32, 128)],
        force, modulus, a, b, s,
    )
    got = [swap(send_a, 1, 0), swap(send_b, 1, 1)]
    got += [swap(far, 3, 0), swap(far, 3, 1, ((0, 2), (top, top - 2)))]
    x, r, far, cm, pc, xc, rc, wc, part = call(
        functools.partial(second_kernel, top),
        [
            (3, 4, 32, 128), (3, 6, 32, 128), (6, 16, 128), (11, 16, 128), (3, 10, 16, 128),
            (3, 2, 16, 128), (3, 8, 16, 128), (3, 8, 16, 128), (n, 1, 128),
        ],
        [(3, 16, 32, 128), (17, 32, 128), (3, 16, 16, 128), (17, 16, 128)],
        force, x, r, m, p, cf, cm, *got,
    )
    got = [swap(far, 2, 0), swap(far, 2, 1, ((0, 1), (top, top - 1)))]
    sums = lax.all_to_all(part, "slab", 0, 0, tiled=True)
    (coarse,) = call(late_kernel, [(3, 2, 16, 64)], [], cm, pc, xc, rc, wc)
    cells = float(modulus.size * n)
    angle = math.acosh(RATIO_C)
    part_way = math.cosh(CDEG * angle)
    full = math.cosh(2 * CDEG * angle)
    scale = (1.0 / cells, 2.0 * part_way * part_way / full / 4.0 / (cells / 8.0))
    fine, total = call(
        functools.partial(third_kernel, top, scale),
        [(3, 4, 32, 128), (2,)],
        [(3, 6, 16, 128)],
        x, r, far, m, p, cm, pc, sums, *got, small=(1,),
    )
    return fine, coarse, total


def solution(mesh):
    return jax.shard_map(
        cycles,
        mesh=mesh,
        in_specs=(P(None, "slab", None, "sample"), P("slab", None, "sample")),
        out_specs=(P(None, "slab", None, "sample"), P(None, "slab", None, "sample"), P("sample")),
        check_vma=False,
    )
```

```python
import functools
import math

import jax
import jax.numpy as jnp
from jax import lax
from jax.experimental import pallas as pl
from jax.experimental.pallas import tpu as pltpu
from jax.sharding import PartitionSpec as P

SMOOTH = 2
CDEG = 4
FINE = (0.25, 2.0)
COARSE = (0.02, 2.0)


def coefficients(low_end, high_end, degree):
    centre = (high_end + low_end) / 2.0
    half = (high_end - low_end) / 2.0
    ratio = centre / half
    rho = 1.0 / ratio
    steps = []
    for _ in range(degree - 1):
        after = 1.0 / (2.0 * ratio - rho)
        steps.append((after * rho, 2.0 * after / half))
        rho = after
    return 1.0 / centre, steps, ratio


FIRST_F, STEPS_F, _ = coefficients(*FINE, SMOOTH)
NOW_F, GAIN_F = STEPS_F[0]
FIRST_C, STEPS_C, RATIO_C = coefficients(*COARSE, 2 * CDEG)


def lanes(shape):
    return lax.broadcasted_iota(jnp.int32, shape, len(shape) - 1)


LINE = (1, 1, 8, 128)


def ahead_x(v, by):
    return jnp.where(lanes(LINE) < 128 - by, pltpu.roll(v, 128 - by, 3), 0.0)


def back_x(v, by):
    return jnp.where(lanes(LINE) >= by, pltpu.roll(v, by, 3), 0.0)


def ahead_y(v):
    at = lax.broadcasted_iota(jnp.int32, LINE, 2)
    moved = jnp.where(at < 7, pltpu.roll(v[:, :1], 7, 2), 0.0)
    return jnp.concatenate([v[:, 1:], moved], 1)


def back_y(v):
    at = lax.broadcasted_iota(jnp.int32, LINE, 2)
    moved = jnp.where(at >= 1, pltpu.roll(v[:, -1:], 1, 2), 0.0)
    return jnp.concatenate([moved, v[:, :-1]], 1)


def operate(u, m, step):
    low = [c[:-1] for c in u]
    gz = [c[1:] - l for c, l in zip(u, low)]
    gx0 = ahead_x(low[0], step) - low[0]
    gy1 = ahead_y(low[1]) - low[1]
    s = m * (gx0 + gy1 + gz[2])
    inner = m[1:]
    si = s[1:]
    out = []
    for c in range(3):
        here = low[c][1:]
        fx = inner * (gx0[1:] if c == 0 else ahead_x(here, step) - here)
        fy = inner * (gy1[1:] if c == 1 else ahead_y(here) - here)
        fz = m * gz[c]
        if c == 0:
            fx = fx + si
        elif c == 1:
            fy = fy + si
        else:
            fz = fz + s
        out.append((fz[:-1] - fz[1:]) + (back_y(fy) - fy) + (back_x(fx, step) - fx))
    return out


def inverse(m, step, scale=1.0):
    here = m[1:]
    below = m[:-1]
    by = back_y(here)
    bx = back_x(here, step)
    lap = (here + below) + (here + by) + (here + bx) + here
    inside = here > 0.0
    return [
        jnp.where(inside, scale / jnp.where(inside, lap + d, 1.0), 0.0) for d in (bx, by, below)
    ]


def trim(v, n=1):
    return v[n : v.shape[0] - n]


def tiles(v):
    return v.reshape(v.shape[0], v.shape[1] // 8, 8, 128)


def rows(v):
    return v.reshape(v.shape[0], v.shape[1] * 8, 128)


def strided(ref, *at):
    return jnp.concatenate([ref[(*at, pl.ds(v, 8, stride=4), slice(None))] for v in range(4)], 0)


def pack(even_sum, odd_sum):
    even = lanes(LINE) % 2 == 0
    near = jnp.where(even, even_sum, odd_sum)
    far = jnp.where(even, pltpu.roll(even_sum, 127, 3), pltpu.roll(odd_sum, 1, 3))
    return near + far


def pair_cells(v):
    out = []
    for i in range(0, v.shape[0], 2):
        t = v[i : i + 1] + v[i + 1 : i + 2]
        out.append(jnp.concatenate([t[:, 0:1] + t[:, 1:2], t[:, 2:3] + t[:, 3:4]], 1))
    return jnp.concatenate(out, 0)


def spread(e, order):
    even = lanes(LINE) % 2 == 0
    both = jnp.where(even, e, pltpu.roll(e, 1, 3))
    wide = jnp.concatenate([both[:, 0:1], both[:, 0:1], both[:, 1:2], both[:, 1:2]], 1)
    return jnp.concatenate([wide[i : i + 1] for i in order], 0)


def by_side(flag, put, a, b):
    lower = flag == 0

    @pl.when(lower)
    def _():
        put(a, b)

    @pl.when(jnp.logical_not(lower))
    def _():
        put(b, a)


def first_kernel(
    f_ref, e_ref, a_ref, b_ref, s_ref,
    x_ref, r_ref, m_ref, p_ref, cf_ref, cm_ref, send_a, send_b, far_ref,
    fe,
):
    for z in range(4):
        for c in range(3):
            fe[c, 4 + z] = strided(f_ref, c, z)
        m_ref[5 + z] = 0.4 * strided(e_ref, z)
    m_ref[0] = 0.4 * strided(s_ref, 0)

    def take(up, down):
        for z in range(4):
            for c in range(3):
                fe[c, 8 + z] = strided(up, 4 * c + z)
                fe[c, z] = strided(down, 4 * c + z)
            m_ref[9 + z] = 0.4 * strided(up, 12 + z)
            m_ref[1 + z] = 0.4 * strided(down, 12 + z)

    me = lax.axis_index("slab")
    by_side(me % 2, take, a_ref, b_ref)
    m = tiles(m_ref[...])
    p = inverse(m, 1, GAIN_F)
    r = [tiles(fe[c]) for c in range(3)]
    w = [p[c] * r[c] * (FIRST_F / GAIN_F) for c in range(3)]
    aw = operate(w, m[1:12], 1)
    f = r
    r = [trim(r[c]) - aw[c] for c in range(3)]
    w2 = [NOW_F * trim(w[c]) + trim(p[c]) * r[c] for c in range(3)]
    aw = operate(w2, m[2:11], 1)
    cm = pair_cells(m[1:13]) * 0.125
    cm = rows(pack(cm, cm))
    cm_ref[...] = cm
    far_ref[12:18] = cm
    for c in range(3):
        p_ref[c] = rows(p[c])
        x_ref[c] = rows(w[c][4:8] + w2[c][3:7])
        done = trim(r[c]) - aw[c]
        r_ref[c] = rows(done)
        both = rows(pack(pair_cells(done) * 0.5, pair_cells(f[c][2:10]) * 0.5))
        cf_ref[c] = both
        far_ref[4 * c : 4 * c + 4] = both
    for ref, q in ((send_a, 0), (send_b, 1)):
        for c in range(3):
            ref[4 * c : 4 * c + 4] = r_ref[c, pl.ds(4 * q, 4)]
            for j in range(2):
                ref[14 + c, 16 * j : 16 * j + 16] = cf_ref[c, 2 * q + j]
        ref[12:14] = m_ref[pl.ds(2 + 7 * q, 2)]


def second_kernel(
    top, f_ref, x_ref, r_ref, m_ref, p_ref, own, own_cm, a1, b1, a3, b3,
    xo_ref, ro_ref, far_ref, cmo_ref, pco_ref, xc_ref, rc_ref, wc_ref, sum_ref,
    re, me, cf, cm,
):
    for c in range(3):
        re[c, 4:12] = r_ref[c]
        cf[c, 6:10] = own[c]
    me[2:15] = m_ref[...]
    cm[6:12] = own_cm[...]

    def near(up, down):
        for c in range(3):
            re[c, 12:16] = up[4 * c : 4 * c + 4]
            re[c, 0:4] = down[4 * c : 4 * c + 4]
            for j in range(2):
                cf[c, 10 + j] = up[14 + c, 16 * j : 16 * j + 16]
                cf[c, 4 + j] = down[14 + c, 16 * j : 16 * j + 16]
        me[15:17] = up[12:14]
        me[0:2] = down[12:14]

    def third(up, down):
        for c in range(3):
            cf[c, 12:16] = up[4 * c : 4 * c + 4]
            cf[c, 0:4] = down[4 * c : 4 * c + 4]
        cm[12:17] = up[12:17]
        cm[0:6] = down[12:18]

    place = lax.axis_index("slab")
    near(a1, b1)

    @pl.when(place == 0)
    def _():
        me[0:2] = jnp.zeros((2, 32, 128), jnp.float32)

    @pl.when(place == top)
    def _():
        me[15:17] = jnp.zeros((2, 32, 128), jnp.float32)

    by_side(half(place, 3), third, a3, b3)

    @pl.when(place == 2)
    def _():
        for c in range(3):
            cf[c, 0:3] = jnp.zeros((3, 16, 128), jnp.float32)
            cf[c, 3] = b3[4 * c + 1]
        cm[0:4] = jnp.zeros((4, 16, 128), jnp.float32)
        cm[4:6] = b3[14:16]

    @pl.when(place == top - 2)
    def _():
        for c in range(3):
            cf[c, 12] = b3[4 * c + 2]
            cf[c, 13:16] = jnp.zeros((3, 16, 128), jnp.float32)
        cm[12:14] = b3[14:16]
        cm[14:17] = jnp.zeros((3, 16, 128), jnp.float32)

    mc = tiles(cm[...])
    pc = inverse(mc, 2)
    r = [tiles(cf[c]) for c in range(3)]
    own_rhs = [t[7:9] for t in r]
    w = [pc[c] * r[c] * FIRST_C for c in range(3)]
    e = [w[c][3:13] for c in range(3)]
    xc = [w[c][7:9] for c in range(3)]
    part = None
    for k in range(1, 5):
        aw = operate(w, mc[k : 17 - k], 2)
        r = [trim(r[c]) - aw[c] for c in range(3)]
        now, gain = STEPS_C[k - 1]
        if k == 4:
            odd = lanes(LINE) % 2 == 1
            part = sum(
                jnp.sum(jnp.where(odd, xc[c] * (own_rhs[c] + r[c][3:5]), 0.0)) for c in range(3)
            )
        w = [now * trim(w[c]) + gain * (pc[c][k : 16 - k] * r[c]) for c in range(3)]
        if k <= 3:
            e = [e[c] + w[c][3 - k : 13 - k] for c in range(3)]
        xc = [xc[c] + w[c][7 - k : 9 - k] for c in range(3)]
    for c in range(3):
        xc_ref[c] = rows(xc[c])
        rc_ref[c] = rows(r[c])
        wc_ref[c] = rows(w[c])
        pco_ref[c] = rows(pc[c][3:13])

    m = tiles(me[...])
    order = [0] + [i for i in range(1, 9) for _ in range(2)] + [9]
    v = [spread(e[c], order) for c in range(3)]
    aw = operate(v, m, 1)
    low = inverse(m[0:3], 1, GAIN_F)
    high = inverse(m[14:17], 1, GAIN_F)
    p = [jnp.concatenate([low[c], tiles(p_ref[c]), high[c]], 0) for c in range(3)]
    r = [tiles(re[c]) - aw[c] for c in range(3)]
    start = FIRST_F / GAIN_F
    w = [p[c] * r[c] * start for c in range(3)]
    x = [tiles(x_ref[c]) + v[c][7:11] + w[c][6:10] for c in range(3)]
    aw = operate(w, m[1:16], 1)
    r = [trim(r[c]) - aw[c] for c in range(3)]
    w = [NOW_F * trim(w[c]) + p[c][1:15] * r[c] for c in range(3)]
    x = [x[c] + w[c][5:9] for c in range(3)]
    aw = operate(w, m[2:15], 1)
    r = [trim(r[c]) - aw[c] for c in range(3)]
    f = [
        jnp.concatenate([strided(f_ref, c, z).reshape(1, 4, 8, 128) for z in range(4)], 0)
        for c in range(3)
    ]
    whole = sum(jnp.sum(x[c] * (f[c] + r[c][4:8])) for c in range(3))
    w = [p[c][2:14] * r[c] * start for c in range(3)]
    x = [x[c] + w[c][4:8] for c in range(3)]
    aw = operate(w, m[3:14], 1)
    r = [trim(r[c]) - aw[c] for c in range(3)]
    w = [NOW_F * trim(w[c]) + p[c][3:13] * r[c] for c in range(3)]
    aw = operate(w, m[4:13], 1)
    for c in range(3):
        xo_ref[c] = rows(x[c] + w[c][3:7])
        done = trim(r[c]) - aw[c]
        ro_ref[c] = rows(done[1:7])
        rc = pair_cells(done) * 0.5
        far_ref[2 * c : 2 * c + 1] = rows(pack(rc[0:1], rc[1:2]))
        far_ref[2 * c + 1 : 2 * c + 2] = rows(pack(rc[2:3], rc[3:4]))
    cmo_ref[...] = cm[3:14]
    at = lanes((1, 128))
    line = jnp.where(at == 0, whole, 0.0) + jnp.where(at == 1, part, 0.0)
    sum_ref[...] = jnp.broadcast_to(line[None], sum_ref.shape)


def late_kernel(cm_ref, pc_ref, xc_ref, rc_ref, wc_ref, coarse_ref):
    mc = tiles(cm_ref[...])
    pc = [tiles(pc_ref[c]) for c in range(3)]
    xc = [tiles(xc_ref[c]) for c in range(3)]
    r = [tiles(rc_ref[c]) for c in range(3)]
    w = [tiles(wc_ref[c]) for c in range(3)]
    for k in range(5, 8):
        aw = operate(w, mc[k - 3 : 14 - k], 2)
        r = [trim(r[c]) - aw[c] for c in range(3)]
        now, gain = STEPS_C[k - 1]
        w = [now * trim(w[c]) + gain * (pc[c][k - 3 : 13 - k] * r[c]) for c in range(3)]
        xc = [xc[c] + w[c][7 - k : 9 - k] for c in range(3)]
    col = lax.broadcasted_iota(jnp.int32, (128, 64), 1)
    row = lax.broadcasted_iota(jnp.int32, (128, 64), 0)
    pick = jnp.where(row == 2 * col + 1, 1.0, 0.0).astype(jnp.float32)
    for c in range(3):
        solved = jnp.dot(
            xc[c].reshape(32, 128), pick,
            precision=lax.Precision.HIGHEST, preferred_element_type=jnp.float32,
        )
        for z in range(2):
            for t in range(2):
                at = 16 * z + 8 * t
                coarse_ref[c, z, pl.ds(t, 8, stride=2), :] = solved[at : at + 8]


def third_kernel(
    top, scale, x_ref, r_ref, own, m_ref, p_ref, cm_ref, pc_ref, sums, a2, b2, out_ref, sum_ref, cf
):
    for c in range(3):
        cf[c, 2:4] = own[2 * c : 2 * c + 2]

    def second(up, down):
        for c in range(3):
            cf[c, 4:6] = up[2 * c : 2 * c + 2]
            cf[c, 0:2] = down[2 * c : 2 * c + 2]

    place = lax.axis_index("slab")
    by_side(half(place, 2), second, a2, b2)
    even = lanes((16, 128)) % 2 == 0

    @pl.when(place == 1)
    def _():
        for c in range(3):
            cf[c, 0] = jnp.zeros((16, 128), jnp.float32)
            cf[c, 1] = jnp.where(even, 0.0, b2[2 * c])

    @pl.when(place == top - 1)
    def _():
        for c in range(3):
            cf[c, 4] = jnp.where(even, b2[2 * c + 1], 0.0)
            cf[c, 5] = jnp.zeros((16, 128), jnp.float32)

    for k in range(2):
        sum_ref[k] = jnp.sum(jnp.where(lanes((64, 1, 128)) == k, sums[...], 0.0)) * scale[k]
    mc = tiles(cm_ref[...])
    pc = [tiles(pc_ref[c]) for c in range(3)]
    r = []
    for c in range(3):
        near = tiles(cf[c])
        far = pltpu.roll(near, 127, 3)
        parts = [t[i : i + 1] for i in range(6) for t in (near, far)]
        r.append(jnp.concatenate(parts[1:11], 0))
    w = [pc[c] * r[c] * FIRST_C for c in range(3)]
    e = [w[c][3:7] for c in range(3)]
    for k in range(1, 4):
        aw = operate(w, mc[k : 11 - k], 2)
        r = [trim(r[c]) - aw[c] for c in range(3)]
        now, gain = STEPS_C[k - 1]
        w = [now * trim(w[c]) + gain * (pc[c][k : 10 - k] * r[c]) for c in range(3)]
        e = [e[c] + w[c][3 - k : 7 - k] for c in range(3)]

    m = tiles(m_ref[3:10])
    order = [0, 0, 1, 1, 2, 2, 3, 3]
    v = [spread(e[c], order) for c in range(3)]
    aw = operate(v, m, 1)
    p = [tiles(p_ref[c, 3:9]) for c in range(3)]
    r = [tiles(r_ref[c]) - aw[c] for c in range(3)]
    w = [p[c] * r[c] * (FIRST_F / GAIN_F) for c in range(3)]
    aw = operate(w, m[1:6], 1)
    for c in range(3):
        after = r[c][1:5] - aw[c]
        x = tiles(x_ref[c]) + v[c][2:6] + (1.0 + NOW_F) * w[c][1:5] + p[c][1:5] * after
        for z in range(4):
            for t in range(4):
                out_ref[c, z, pl.ds(t, 8, stride=4), :] = x[z, t]


def call(kernel, outs, scratch, *args, small=(), flops=1 << 22):
    places = [pltpu.SMEM if i in small else pltpu.VMEM for i in range(len(outs))]
    return pl.pallas_call(
        kernel,
        out_shape=[jax.ShapeDtypeStruct(s, jnp.float32) for s in outs],
        in_specs=[pl.BlockSpec(memory_space=pltpu.VMEM)] * len(args),
        out_specs=[pl.BlockSpec(memory_space=place) for place in places],
        scratch_shapes=[pltpu.VMEM(s, jnp.float32) for s in scratch],
        compiler_params=pltpu.CompilerParams(vmem_limit_bytes=16 << 20),
        cost_estimate=pl.CostEstimate(flops=flops, bytes_accessed=1 << 20, transcendentals=0),
    )(*args)


def half(i, distance):
    if distance == 3:
        i = i + 3 * (i % 3) * (2 - i % 3)
    return (i // distance) % 2


def swap(x, distance, second, extra=(), axis="slab"):
    n = lax.axis_size(axis)
    pairs = list(extra)
    for i in range(n - distance):
        if half(i, distance) == second:
            pairs += [(i, i + distance), (i + distance, i)]
    return lax.ppermute(x, axis, pairs)


def shift(x, by, axis="slab"):
    n = lax.axis_size(axis)
    return lax.ppermute(x, axis, [(i, (i + by) % n) for i in range(n)])


def cycles(force, modulus):
    n = lax.axis_size("slab")
    top = n - 1
    if half(top, 3) != 1 or half(top - 2, 3) != 1 or half(top, 2) != 1:
        raise ValueError("slab count")
    block = jnp.concatenate([force.reshape(12, 32, 128), modulus], 0)
    a = swap(block, 1, 0)
    b = swap(block, 1, 1)
    s = lax.ppermute(modulus[3:4], "slab", [(i, i + 2) for i in range(n - 2)])
    x, r, m, p, cf, cm, send_a, send_b, far = call(
        first_kernel,
        [
            (3, 4, 32, 128), (3, 8, 32, 128), (13, 32, 128), (3, 12, 32, 128), (3, 4, 16, 128),
            (6, 16, 128), (17, 32, 128), (17, 32, 128), (18, 16, 128),
        ],
        [(3, 12, 32, 128)],
        force, modulus, a, b, s,
    )
    got = [shift(send_b, -1), shift(send_a, 1)]
    got += [swap(far, 3, 0), swap(far, 3, 1, ((0, 2), (top, top - 2)))]
    x, r, far, cm, pc, xc, rc, wc, part = call(
        functools.partial(second_kernel, top),
        [
            (3, 4, 32, 128), (3, 6, 32, 128), (6, 16, 128), (11, 16, 128), (3, 10, 16, 128),
            (3, 2, 16, 128), (3, 8, 16, 128), (3, 8, 16, 128), (n, 1, 128),
        ],
        [(3, 16, 32, 128), (17, 32, 128), (3, 16, 16, 128), (17, 16, 128)],
        force, x, r, m, p, cf, cm, *got,
    )
    got = [swap(far, 2, 0), swap(far, 2, 1, ((0, 1), (top, top - 1)))]
    sums = lax.all_to_all(part, "slab", 0, 0, tiled=True)
    (coarse,) = call(late_kernel, [(3, 2, 16, 64)], [], cm, pc, xc, rc, wc)
    cells = float(modulus.size * n)
    angle = math.acosh(RATIO_C)
    part_way = math.cosh(CDEG * angle)
    full = math.cosh(2 * CDEG * angle)
    scale = (1.0 / cells, 2.0 * part_way * part_way / full / 4.0 / (cells / 8.0))
    fine, total = call(
        functools.partial(third_kernel, top, scale),
        [(3, 4, 32, 128), (2,)],
        [(3, 6, 16, 128)],
        x, r, far, m, p, cm, pc, sums, *got, small=(1,),
    )
    return fine, coarse, total


def solution(mesh):
    return jax.shard_map(
        cycles,
        mesh=mesh,
        in_specs=(P(None, "slab", None, "sample"), P("slab", None, "sample")),
        out_specs=(P(None, "slab", None, "sample"), P(None, "slab", None, "sample"), P("sample")),
        check_vma=False,
    )
```

```python
import functools
import math

import jax
import jax.numpy as jnp
from jax import lax
from jax.experimental import pallas as pl
from jax.experimental.pallas import tpu as pltpu
from jax.sharding import PartitionSpec as P

SMOOTH = 2
CDEG = 4
FINE = (0.25, 2.0)
COARSE = (0.02, 2.0)


def coefficients(low_end, high_end, degree):
    centre = (high_end + low_end) / 2.0
    half = (high_end - low_end) / 2.0
    ratio = centre / half
    rho = 1.0 / ratio
    steps = []
    for _ in range(degree - 1):
        after = 1.0 / (2.0 * ratio - rho)
        steps.append((after * rho, 2.0 * after / half))
        rho = after
    return 1.0 / centre, steps, ratio


FIRST_F, STEPS_F, _ = coefficients(*FINE, SMOOTH)
NOW_F, GAIN_F = STEPS_F[0]
FIRST_C, STEPS_C, RATIO_C = coefficients(*COARSE, 2 * CDEG)


def lanes(shape):
    return lax.broadcasted_iota(jnp.int32, shape, len(shape) - 1)


LINE = (1, 1, 8, 128)


def ahead_x(v, by):
    return jnp.where(lanes(LINE) < 128 - by, pltpu.roll(v, 128 - by, 3), 0.0)


def back_x(v, by):
    return jnp.where(lanes(LINE) >= by, pltpu.roll(v, by, 3), 0.0)


def ahead_y(v):
    at = lax.broadcasted_iota(jnp.int32, LINE, 2)
    moved = jnp.where(at < 7, pltpu.roll(v[:, :1], 7, 2), 0.0)
    return jnp.concatenate([v[:, 1:], moved], 1)


def back_y(v):
    at = lax.broadcasted_iota(jnp.int32, LINE, 2)
    moved = jnp.where(at >= 1, pltpu.roll(v[:, -1:], 1, 2), 0.0)
    return jnp.concatenate([moved, v[:, :-1]], 1)


def operate(u, m, step):
    low = [c[:-1] for c in u]
    gz = [c[1:] - l for c, l in zip(u, low)]
    gx0 = ahead_x(low[0], step) - low[0]
    gy1 = ahead_y(low[1]) - low[1]
    s = m * (gx0 + gy1 + gz[2])
    inner = m[1:]
    si = s[1:]
    out = []
    for c in range(3):
        here = low[c][1:]
        fx = inner * (gx0[1:] if c == 0 else ahead_x(here, step) - here)
        fy = inner * (gy1[1:] if c == 1 else ahead_y(here) - here)
        fz = m * gz[c]
        if c == 0:
            fx = fx + si
        elif c == 1:
            fy = fy + si
        else:
            fz = fz + s
        out.append((fz[:-1] - fz[1:]) + (back_y(fy) - fy) + (back_x(fx, step) - fx))
    return out


def inverse(m, step, scale=1.0):
    here = m[1:]
    below = m[:-1]
    by = back_y(here)
    bx = back_x(here, step)
    lap = (here + below) + (here + by) + (here + bx) + here
    inside = here > 0.0
    return [
        jnp.where(inside, scale / jnp.where(inside, lap + d, 1.0), 0.0) for d in (bx, by, below)
    ]


def trim(v, n=1):
    return v[n : v.shape[0] - n]


def tiles(v):
    return v.reshape(v.shape[0], v.shape[1] // 8, 8, 128)


def rows(v):
    return v.reshape(v.shape[0], v.shape[1] * 8, 128)


def strided(ref, *at):
    return jnp.concatenate([ref[(*at, pl.ds(v, 8, stride=4), slice(None))] for v in range(4)], 0)


def pack(even_sum, odd_sum):
    even = lanes(LINE) % 2 == 0
    near = jnp.where(even, even_sum, odd_sum)
    far = jnp.where(even, pltpu.roll(even_sum, 127, 3), pltpu.roll(odd_sum, 1, 3))
    return near + far


def pair_cells(v):
    out = []
    for i in range(0, v.shape[0], 2):
        t = v[i : i + 1] + v[i + 1 : i + 2]
        out.append(jnp.concatenate([t[:, 0:1] + t[:, 1:2], t[:, 2:3] + t[:, 3:4]], 1))
    return jnp.concatenate(out, 0)


def spread(e, order):
    even = lanes(LINE) % 2 == 0
    both = jnp.where(even, e, pltpu.roll(e, 1, 3))
    wide = jnp.concatenate([both[:, 0:1], both[:, 0:1], both[:, 1:2], both[:, 1:2]], 1)
    return jnp.concatenate([wide[i : i + 1] for i in order], 0)


def by_side(flag, put, a, b):
    lower = flag == 0

    @pl.when(lower)
    def _():
        put(a, b)

    @pl.when(jnp.logical_not(lower))
    def _():
        put(b, a)


def first_kernel(
    top, f_ref, e_ref, a_ref, b_ref, s_ref,
    x_ref, r_ref, m_ref, p_ref, cf_ref, cm_ref, send_a, send_b, far_ref,
    fe,
):
    for z in range(4):
        for c in range(3):
            fe[c, 4 + z] = strided(f_ref, c, z)
        m_ref[5 + z] = 0.4 * strided(e_ref, z)
    m_ref[0] = 0.4 * strided(s_ref, 0)

    def take(up, down):
        for z in range(4):
            for c in range(3):
                fe[c, 8 + z] = strided(up, 4 * c + z)
                fe[c, z] = strided(down, 4 * c + z)
            m_ref[9 + z] = 0.4 * strided(up, 12 + z)
            m_ref[1 + z] = 0.4 * strided(down, 12 + z)

    me = lax.axis_index("slab")
    take(a_ref, b_ref)

    @pl.when(me == 0)
    def _():
        m_ref[0:5] = jnp.zeros((5, 32, 128), jnp.float32)

    @pl.when(me == top)
    def _():
        m_ref[9:13] = jnp.zeros((4, 32, 128), jnp.float32)

    m = tiles(m_ref[...])
    p = inverse(m, 1, GAIN_F)
    r = [tiles(fe[c]) for c in range(3)]
    w = [p[c] * r[c] * (FIRST_F / GAIN_F) for c in range(3)]
    aw = operate(w, m[1:12], 1)
    f = r
    r = [trim(r[c]) - aw[c] for c in range(3)]
    w2 = [NOW_F * trim(w[c]) + trim(p[c]) * r[c] for c in range(3)]
    aw = operate(w2, m[2:11], 1)
    cm = pair_cells(m[1:13]) * 0.125
    cm = rows(pack(cm, cm))
    cm_ref[...] = cm
    far_ref[12:18] = cm
    for c in range(3):
        p_ref[c] = rows(p[c])
        x_ref[c] = rows(w[c][4:8] + w2[c][3:7])
        done = trim(r[c]) - aw[c]
        r_ref[c] = rows(done)
        both = rows(pack(pair_cells(done) * 0.5, pair_cells(f[c][2:10]) * 0.5))
        cf_ref[c] = both
        far_ref[4 * c : 4 * c + 4] = both
    for ref, q in ((send_a, 0), (send_b, 1)):
        for c in range(3):
            ref[4 * c : 4 * c + 4] = r_ref[c, pl.ds(4 * q, 4)]
            for j in range(2):
                ref[14 + c, 16 * j : 16 * j + 16] = cf_ref[c, 2 * q + j]
        ref[12:14] = m_ref[pl.ds(2 + 7 * q, 2)]


def second_kernel(
    top, f_ref, x_ref, r_ref, m_ref, p_ref, own, own_cm, a1, b1, a3, b3,
    xo_ref, ro_ref, far_ref, cmo_ref, pco_ref, xc_ref, rc_ref, wc_ref, sum_ref,
    re, me, cf, cm,
):
    for c in range(3):
        re[c, 4:12] = r_ref[c]
        cf[c, 6:10] = own[c]
    me[2:15] = m_ref[...]
    cm[6:12] = own_cm[...]

    def near(up, down):
        for c in range(3):
            re[c, 12:16] = up[4 * c : 4 * c + 4]
            re[c, 0:4] = down[4 * c : 4 * c + 4]
            for j in range(2):
                cf[c, 10 + j] = up[14 + c, 16 * j : 16 * j + 16]
                cf[c, 4 + j] = down[14 + c, 16 * j : 16 * j + 16]
        me[15:17] = up[12:14]
        me[0:2] = down[12:14]

    def third(up, down):
        for c in range(3):
            cf[c, 12:16] = up[4 * c : 4 * c + 4]
            cf[c, 0:4] = down[4 * c : 4 * c + 4]
        cm[12:17] = up[12:17]
        cm[0:6] = down[12:18]

    place = lax.axis_index("slab")
    near(a1, b1)

    @pl.when(place == 0)
    def _():
        me[0:2] = jnp.zeros((2, 32, 128), jnp.float32)

    @pl.when(place == top)
    def _():
        me[15:17] = jnp.zeros((2, 32, 128), jnp.float32)

    by_side(half(place, 3), third, a3, b3)

    @pl.when(place == 2)
    def _():
        for c in range(3):
            cf[c, 0:3] = jnp.zeros((3, 16, 128), jnp.float32)
            cf[c, 3] = b3[4 * c + 1]
        cm[0:4] = jnp.zeros((4, 16, 128), jnp.float32)
        cm[4:6] = b3[14:16]

    @pl.when(place == top - 2)
    def _():
        for c in range(3):
            cf[c, 12] = b3[4 * c + 2]
            cf[c, 13:16] = jnp.zeros((3, 16, 128), jnp.float32)
        cm[12:14] = b3[14:16]
        cm[14:17] = jnp.zeros((3, 16, 128), jnp.float32)

    mc = tiles(cm[...])
    pc = inverse(mc, 2)
    r = [tiles(cf[c]) for c in range(3)]
    own_rhs = [t[7:9] for t in r]
    w = [pc[c] * r[c] * FIRST_C for c in range(3)]
    e = [w[c][3:13] for c in range(3)]
    xc = [w[c][7:9] for c in range(3)]
    part = None
    for k in range(1, 5):
        aw = operate(w, mc[k : 17 - k], 2)
        r = [trim(r[c]) - aw[c] for c in range(3)]
        now, gain = STEPS_C[k - 1]
        if k == 4:
            odd = lanes(LINE) % 2 == 1
            part = sum(
                jnp.sum(jnp.where(odd, xc[c] * (own_rhs[c] + r[c][3:5]), 0.0)) for c in range(3)
            )
        w = [now * trim(w[c]) + gain * (pc[c][k : 16 - k] * r[c]) for c in range(3)]
        if k <= 3:
            e = [e[c] + w[c][3 - k : 13 - k] for c in range(3)]
        xc = [xc[c] + w[c][7 - k : 9 - k] for c in range(3)]
    for c in range(3):
        xc_ref[c] = rows(xc[c])
        rc_ref[c] = rows(r[c])
        wc_ref[c] = rows(w[c])
        pco_ref[c] = rows(pc[c][3:13])

    m = tiles(me[...])
    order = [0] + [i for i in range(1, 9) for _ in range(2)] + [9]
    v = [spread(e[c], order) for c in range(3)]
    aw = operate(v, m, 1)
    low = inverse(m[0:3], 1, GAIN_F)
    high = inverse(m[14:17], 1, GAIN_F)
    p = [jnp.concatenate([low[c], tiles(p_ref[c]), high[c]], 0) for c in range(3)]
    r = [tiles(re[c]) - aw[c] for c in range(3)]
    start = FIRST_F / GAIN_F
    w = [p[c] * r[c] * start for c in range(3)]
    x = [tiles(x_ref[c]) + v[c][7:11] + w[c][6:10] for c in range(3)]
    aw = operate(w, m[1:16], 1)
    r = [trim(r[c]) - aw[c] for c in range(3)]
    w = [NOW_F * trim(w[c]) + p[c][1:15] * r[c] for c in range(3)]
    x = [x[c] + w[c][5:9] for c in range(3)]
    aw = operate(w, m[2:15], 1)
    r = [trim(r[c]) - aw[c] for c in range(3)]
    f = [
        jnp.concatenate([strided(f_ref, c, z).reshape(1, 4, 8, 128) for z in range(4)], 0)
        for c in range(3)
    ]
    whole = sum(jnp.sum(x[c] * (f[c] + r[c][4:8])) for c in range(3))
    w = [p[c][2:14] * r[c] * start for c in range(3)]
    x = [x[c] + w[c][4:8] for c in range(3)]
    aw = operate(w, m[3:14], 1)
    r = [trim(r[c]) - aw[c] for c in range(3)]
    w = [NOW_F * trim(w[c]) + p[c][3:13] * r[c] for c in range(3)]
    aw = operate(w, m[4:13], 1)
    for c in range(3):
        xo_ref[c] = rows(x[c] + w[c][3:7])
        done = trim(r[c]) - aw[c]
        ro_ref[c] = rows(done[1:7])
        rc = pair_cells(done) * 0.5
        far_ref[2 * c : 2 * c + 1] = rows(pack(rc[0:1], rc[1:2]))
        far_ref[2 * c + 1 : 2 * c + 2] = rows(pack(rc[2:3], rc[3:4]))
    cmo_ref[...] = cm[3:14]
    at = lanes((1, 128))
    line = jnp.where(at == 0, whole, 0.0) + jnp.where(at == 1, part, 0.0)
    sum_ref[...] = jnp.broadcast_to(line[None], sum_ref.shape)


def late_kernel(cm_ref, pc_ref, xc_ref, rc_ref, wc_ref, coarse_ref):
    mc = tiles(cm_ref[...])
    pc = [tiles(pc_ref[c]) for c in range(3)]
    xc = [tiles(xc_ref[c]) for c in range(3)]
    r = [tiles(rc_ref[c]) for c in range(3)]
    w = [tiles(wc_ref[c]) for c in range(3)]
    for k in range(5, 8):
        aw = operate(w, mc[k - 3 : 14 - k], 2)
        r = [trim(r[c]) - aw[c] for c in range(3)]
        now, gain = STEPS_C[k - 1]
        w = [now * trim(w[c]) + gain * (pc[c][k - 3 : 13 - k] * r[c]) for c in range(3)]
        xc = [xc[c] + w[c][7 - k : 9 - k] for c in range(3)]
    col = lax.broadcasted_iota(jnp.int32, (128, 64), 1)
    row = lax.broadcasted_iota(jnp.int32, (128, 64), 0)
    pick = jnp.where(row == 2 * col + 1, 1.0, 0.0).astype(jnp.float32)
    for c in range(3):
        solved = jnp.dot(
            xc[c].reshape(32, 128), pick,
            precision=lax.Precision.HIGHEST, preferred_element_type=jnp.float32,
        )
        for z in range(2):
            for t in range(2):
                at = 16 * z + 8 * t
                coarse_ref[c, z, pl.ds(t, 8, stride=2), :] = solved[at : at + 8]


def third_kernel(
    top, scale, x_ref, r_ref, own, m_ref, p_ref, cm_ref, pc_ref, sums, a2, b2, out_ref, sum_ref, cf
):
    for c in range(3):
        cf[c, 2:4] = own[2 * c : 2 * c + 2]

    def second(up, down):
        for c in range(3):
            cf[c, 4:6] = up[2 * c : 2 * c + 2]
            cf[c, 0:2] = down[2 * c : 2 * c + 2]

    place = lax.axis_index("slab")
    by_side(half(place, 2), second, a2, b2)
    even = lanes((16, 128)) % 2 == 0

    @pl.when(place == 1)
    def _():
        for c in range(3):
            cf[c, 0] = jnp.zeros((16, 128), jnp.float32)
            cf[c, 1] = jnp.where(even, 0.0, b2[2 * c])

    @pl.when(place == top - 1)
    def _():
        for c in range(3):
            cf[c, 4] = jnp.where(even, b2[2 * c + 1], 0.0)
            cf[c, 5] = jnp.zeros((16, 128), jnp.float32)

    for k in range(2):
        sum_ref[k] = jnp.sum(jnp.where(lanes((64, 1, 128)) == k, sums[...], 0.0)) * scale[k]
    mc = tiles(cm_ref[...])
    pc = [tiles(pc_ref[c]) for c in range(3)]
    r = []
    for c in range(3):
        near = tiles(cf[c])
        far = pltpu.roll(near, 127, 3)
        parts = [t[i : i + 1] for i in range(6) for t in (near, far)]
        r.append(jnp.concatenate(parts[1:11], 0))
    w = [pc[c] * r[c] * FIRST_C for c in range(3)]
    e = [w[c][3:7] for c in range(3)]
    for k in range(1, 4):
        aw = operate(w, mc[k : 11 - k], 2)
        r = [trim(r[c]) - aw[c] for c in range(3)]
        now, gain = STEPS_C[k - 1]
        w = [now * trim(w[c]) + gain * (pc[c][k : 10 - k] * r[c]) for c in range(3)]
        e = [e[c] + w[c][3 - k : 7 - k] for c in range(3)]

    m = tiles(m_ref[3:10])
    order = [0, 0, 1, 1, 2, 2, 3, 3]
    v = [spread(e[c], order) for c in range(3)]
    aw = operate(v, m, 1)
    p = [tiles(p_ref[c, 3:9]) for c in range(3)]
    r = [tiles(r_ref[c]) - aw[c] for c in range(3)]
    w = [p[c] * r[c] * (FIRST_F / GAIN_F) for c in range(3)]
    aw = operate(w, m[1:6], 1)
    for c in range(3):
        after = r[c][1:5] - aw[c]
        x = tiles(x_ref[c]) + v[c][2:6] + (1.0 + NOW_F) * w[c][1:5] + p[c][1:5] * after
        for z in range(4):
            for t in range(4):
                out_ref[c, z, pl.ds(t, 8, stride=4), :] = x[z, t]


def call(kernel, outs, scratch, *args, small=(), flops=1 << 22):
    places = [pltpu.SMEM if i in small else pltpu.VMEM for i in range(len(outs))]
    return pl.pallas_call(
        kernel,
        out_shape=[jax.ShapeDtypeStruct(s, jnp.float32) for s in outs],
        in_specs=[pl.BlockSpec(memory_space=pltpu.VMEM)] * len(args),
        out_specs=[pl.BlockSpec(memory_space=place) for place in places],
        scratch_shapes=[pltpu.VMEM(s, jnp.float32) for s in scratch],
        compiler_params=pltpu.CompilerParams(vmem_limit_bytes=16 << 20),
        cost_estimate=pl.CostEstimate(flops=flops, bytes_accessed=1 << 20, transcendentals=0),
    )(*args)


def half(i, distance):
    if distance == 3:
        i = i + 3 * (i % 3) * (2 - i % 3)
    return (i // distance) % 2


def swap(x, distance, second, extra=(), axis="slab"):
    n = lax.axis_size(axis)
    pairs = list(extra)
    for i in range(n - distance):
        if half(i, distance) == second:
            pairs += [(i, i + distance), (i + distance, i)]
    return lax.ppermute(x, axis, pairs)


def shift(x, by, axis="slab"):
    n = lax.axis_size(axis)
    return lax.ppermute(x, axis, [(i, (i + by) % n) for i in range(n)])


def cycles(force, modulus):
    n = lax.axis_size("slab")
    top = n - 1
    if half(top, 3) != 1 or half(top - 2, 3) != 1 or half(top, 2) != 1:
        raise ValueError("slab count")
    block = jnp.concatenate([force.reshape(12, 32, 128), modulus], 0)
    a = shift(block, -1)
    b = shift(block, 1)
    s = lax.ppermute(modulus[3:4], "slab", [(i, i + 2) for i in range(n - 2)])
    x, r, m, p, cf, cm, send_a, send_b, far = call(
        functools.partial(first_kernel, top),
        [
            (3, 4, 32, 128), (3, 8, 32, 128), (13, 32, 128), (3, 12, 32, 128), (3, 4, 16, 128),
            (6, 16, 128), (17, 32, 128), (17, 32, 128), (18, 16, 128),
        ],
        [(3, 12, 32, 128)],
        force, modulus, a, b, s,
    )
    got = [shift(send_b, -1), shift(send_a, 1)]
    got += [swap(far, 3, 0), swap(far, 3, 1, ((0, 2), (top, top - 2)))]
    x, r, far, cm, pc, xc, rc, wc, part = call(
        functools.partial(second_kernel, top),
        [
            (3, 4, 32, 128), (3, 6, 32, 128), (6, 16, 128), (11, 16, 128), (3, 10, 16, 128),
            (3, 2, 16, 128), (3, 8, 16, 128), (3, 8, 16, 128), (n, 1, 128),
        ],
        [(3, 16, 32, 128), (17, 32, 128), (3, 16, 16, 128), (17, 16, 128)],
        force, x, r, m, p, cf, cm, *got,
    )
    got = [swap(far, 2, 0), swap(far, 2, 1, ((0, 1), (top, top - 1)))]
    sums = lax.all_to_all(part, "slab", 0, 0, tiled=True)
    (coarse,) = call(late_kernel, [(3, 2, 16, 64)], [], cm, pc, xc, rc, wc)
    cells = float(modulus.size * n)
    angle = math.acosh(RATIO_C)
    part_way = math.cosh(CDEG * angle)
    full = math.cosh(2 * CDEG * angle)
    scale = (1.0 / cells, 2.0 * part_way * part_way / full / 4.0 / (cells / 8.0))
    fine, total = call(
        functools.partial(third_kernel, top, scale),
        [(3, 4, 32, 128), (2,)],
        [(3, 6, 16, 128)],
        x, r, far, m, p, cm, pc, sums, *got, small=(1,),
    )
    return fine, coarse, total


def solution(mesh):
    return jax.shard_map(
        cycles,
        mesh=mesh,
        in_specs=(P(None, "slab", None, "sample"), P("slab", None, "sample")),
        out_specs=(P(None, "slab", None, "sample"), P(None, "slab", None, "sample"), P("sample")),
        check_vma=False,
    )
```

```python
import functools
import math

import jax
import jax.numpy as jnp
from jax import lax
from jax.experimental import pallas as pl
from jax.experimental.pallas import tpu as pltpu
from jax.sharding import PartitionSpec as P

SMOOTH = 2
CDEG = 4
FINE = (0.25, 2.0)
COARSE = (0.02, 2.0)


def coefficients(low_end, high_end, degree):
    centre = (high_end + low_end) / 2.0
    half = (high_end - low_end) / 2.0
    ratio = centre / half
    rho = 1.0 / ratio
    steps = []
    for _ in range(degree - 1):
        after = 1.0 / (2.0 * ratio - rho)
        steps.append((after * rho, 2.0 * after / half))
        rho = after
    return 1.0 / centre, steps, ratio


FIRST_F, STEPS_F, _ = coefficients(*FINE, SMOOTH)
NOW_F, GAIN_F = STEPS_F[0]
FIRST_C, STEPS_C, RATIO_C = coefficients(*COARSE, 2 * CDEG)


def lanes(shape):
    return lax.broadcasted_iota(jnp.int32, shape, len(shape) - 1)


LINE = (1, 1, 8, 128)


def ahead_x(v, by):
    return jnp.where(lanes(LINE) < 128 - by, pltpu.roll(v, 128 - by, 3), 0.0)


def back_x(v, by):
    return jnp.where(lanes(LINE) >= by, pltpu.roll(v, by, 3), 0.0)


def ahead_y(v):
    at = lax.broadcasted_iota(jnp.int32, LINE, 2)
    moved = jnp.where(at < 7, pltpu.roll(v[:, :1], 7, 2), 0.0)
    return jnp.concatenate([v[:, 1:], moved], 1)


def back_y(v):
    at = lax.broadcasted_iota(jnp.int32, LINE, 2)
    moved = jnp.where(at >= 1, pltpu.roll(v[:, -1:], 1, 2), 0.0)
    return jnp.concatenate([moved, v[:, :-1]], 1)


def operate(u, m, step):
    low = [c[:-1] for c in u]
    gz = [c[1:] - l for c, l in zip(u, low)]
    gx0 = ahead_x(low[0], step) - low[0]
    gy1 = ahead_y(low[1]) - low[1]
    s = m * (gx0 + gy1 + gz[2])
    inner = m[1:]
    si = s[1:]
    out = []
    for c in range(3):
        here = low[c][1:]
        fx = inner * (gx0[1:] if c == 0 else ahead_x(here, step) - here)
        fy = inner * (gy1[1:] if c == 1 else ahead_y(here) - here)
        fz = m * gz[c]
        if c == 0:
            fx = fx + si
        elif c == 1:
            fy = fy + si
        else:
            fz = fz + s
        out.append((fz[:-1] - fz[1:]) + (back_y(fy) - fy) + (back_x(fx, step) - fx))
    return out


def inverse(m, step, scale=1.0):
    here = m[1:]
    below = m[:-1]
    by = back_y(here)
    bx = back_x(here, step)
    lap = (here + below) + (here + by) + (here + bx) + here
    inside = here > 0.0
    lap = jnp.where(inside, lap, 1.0)
    top = jnp.where(inside, scale, 0.0)
    return [top / (lap + d) for d in (bx, by, below)]


def trim(v, n=1):
    return v[n : v.shape[0] - n]


def tiles(v):
    return v.reshape(v.shape[0], v.shape[1] // 8, 8, 128)


def rows(v):
    return v.reshape(v.shape[0], v.shape[1] * 8, 128)


def strided(ref, *at):
    return jnp.concatenate([ref[(*at, pl.ds(v, 8, stride=4), slice(None))] for v in range(4)], 0)


def pack(even_sum, odd_sum):
    even = lanes(LINE) % 2 == 0
    near = jnp.where(even, even_sum, odd_sum)
    far = jnp.where(even, pltpu.roll(even_sum, 127, 3), pltpu.roll(odd_sum, 1, 3))
    return near + far


def pair_cells(v):
    out = []
    for i in range(0, v.shape[0], 2):
        t = v[i : i + 1] + v[i + 1 : i + 2]
        out.append(jnp.concatenate([t[:, 0:1] + t[:, 1:2], t[:, 2:3] + t[:, 3:4]], 1))
    return jnp.concatenate(out, 0)


def spread(e, order):
    even = lanes(LINE) % 2 == 0
    both = jnp.where(even, e, pltpu.roll(e, 1, 3))
    wide = jnp.concatenate([both[:, 0:1], both[:, 0:1], both[:, 1:2], both[:, 1:2]], 1)
    return jnp.concatenate([wide[i : i + 1] for i in order], 0)


def by_side(flag, put, a, b):
    lower = flag == 0

    @pl.when(lower)
    def _():
        put(a, b)

    @pl.when(jnp.logical_not(lower))
    def _():
        put(b, a)


def first_kernel(
    top, f_ref, e_ref, a_ref, b_ref, s_ref,
    x_ref, r_ref, m_ref, p_ref, cf_ref, cm_ref, send_a, send_b, far_ref,
    fe,
):
    for z in range(4):
        for c in range(3):
            fe[c, 4 + z] = strided(f_ref, c, z)
        m_ref[5 + z] = 0.4 * strided(e_ref, z)
    m_ref[0] = 0.4 * strided(s_ref, 0)

    def take(up, down):
        for z in range(4):
            for c in range(3):
                fe[c, 8 + z] = strided(up, 4 * c + z)
                fe[c, z] = strided(down, 4 * c + z)
            m_ref[9 + z] = 0.4 * strided(up, 12 + z)
            m_ref[1 + z] = 0.4 * strided(down, 12 + z)

    me = lax.axis_index("slab")
    take(a_ref, b_ref)

    @pl.when(me == 0)
    def _():
        m_ref[0:5] = jnp.zeros((5, 32, 128), jnp.float32)

    @pl.when(me == top)
    def _():
        m_ref[9:13] = jnp.zeros((4, 32, 128), jnp.float32)

    m = tiles(m_ref[...])
    p = inverse(m, 1, GAIN_F)
    r = [tiles(fe[c]) for c in range(3)]
    w = [p[c] * r[c] * (FIRST_F / GAIN_F) for c in range(3)]
    aw = operate(w, m[1:12], 1)
    f = r
    r = [trim(r[c]) - aw[c] for c in range(3)]
    w2 = [NOW_F * trim(w[c]) + trim(p[c]) * r[c] for c in range(3)]
    aw = operate(w2, m[2:11], 1)
    cm = pair_cells(m[1:13]) * 0.125
    cm = rows(pack(cm, cm))
    cm_ref[...] = cm
    far_ref[12:18] = cm
    for c in range(3):
        p_ref[c] = rows(p[c])
        x_ref[c] = rows(w[c][4:8] + w2[c][3:7])
        done = trim(r[c]) - aw[c]
        r_ref[c] = rows(done)
        both = rows(pack(pair_cells(done) * 0.5, pair_cells(f[c][2:10]) * 0.5))
        cf_ref[c] = both
        far_ref[4 * c : 4 * c + 4] = both
    for ref, q in ((send_a, 0), (send_b, 1)):
        for c in range(3):
            ref[4 * c : 4 * c + 4] = r_ref[c, pl.ds(4 * q, 4)]
            for j in range(2):
                ref[14 + c, 16 * j : 16 * j + 16] = cf_ref[c, 2 * q + j]
        ref[12:14] = m_ref[pl.ds(2 + 7 * q, 2)]


def second_kernel(
    top, f_ref, x_ref, r_ref, m_ref, p_ref, own, own_cm, a1, b1, a3, b3,
    xo_ref, ro_ref, far_ref, cmo_ref, pco_ref, xc_ref, rc_ref, wc_ref, sum_ref,
    re, me, cf, cm,
):
    for c in range(3):
        re[c, 4:12] = r_ref[c]
        cf[c, 6:10] = own[c]
    me[2:15] = m_ref[...]
    cm[6:12] = own_cm[...]

    def near(up, down):
        for c in range(3):
            re[c, 12:16] = up[4 * c : 4 * c + 4]
            re[c, 0:4] = down[4 * c : 4 * c + 4]
            for j in range(2):
                cf[c, 10 + j] = up[14 + c, 16 * j : 16 * j + 16]
                cf[c, 4 + j] = down[14 + c, 16 * j : 16 * j + 16]
        me[15:17] = up[12:14]
        me[0:2] = down[12:14]

    def third(up, down):
        for c in range(3):
            cf[c, 12:16] = up[4 * c : 4 * c + 4]
            cf[c, 0:4] = down[4 * c : 4 * c + 4]
        cm[12:17] = up[12:17]
        cm[0:6] = down[12:18]

    place = lax.axis_index("slab")
    near(a1, b1)

    @pl.when(place == 0)
    def _():
        me[0:2] = jnp.zeros((2, 32, 128), jnp.float32)

    @pl.when(place == top)
    def _():
        me[15:17] = jnp.zeros((2, 32, 128), jnp.float32)

    by_side(half(place, 3), third, a3, b3)

    @pl.when(place == 2)
    def _():
        for c in range(3):
            cf[c, 0:3] = jnp.zeros((3, 16, 128), jnp.float32)
            cf[c, 3] = b3[4 * c + 1]
        cm[0:4] = jnp.zeros((4, 16, 128), jnp.float32)
        cm[4:6] = b3[14:16]

    @pl.when(place == top - 2)
    def _():
        for c in range(3):
            cf[c, 12] = b3[4 * c + 2]
            cf[c, 13:16] = jnp.zeros((3, 16, 128), jnp.float32)
        cm[12:14] = b3[14:16]
        cm[14:17] = jnp.zeros((3, 16, 128), jnp.float32)

    mc = tiles(cm[...])
    pc = inverse(mc, 2)
    r = [tiles(cf[c]) for c in range(3)]
    own_rhs = [t[7:9] for t in r]
    w = [pc[c] * r[c] * FIRST_C for c in range(3)]
    e = [w[c][3:13] for c in range(3)]
    xc = [w[c][7:9] for c in range(3)]
    part = None
    for k in range(1, 5):
        aw = operate(w, mc[k : 17 - k], 2)
        r = [trim(r[c]) - aw[c] for c in range(3)]
        now, gain = STEPS_C[k - 1]
        if k == 4:
            odd = lanes(LINE) % 2 == 1
            part = sum(
                jnp.sum(jnp.where(odd, xc[c] * (own_rhs[c] + r[c][3:5]), 0.0)) for c in range(3)
            )
        w = [now * trim(w[c]) + gain * (pc[c][k : 16 - k] * r[c]) for c in range(3)]
        if k <= 3:
            e = [e[c] + w[c][3 - k : 13 - k] for c in range(3)]
        xc = [xc[c] + w[c][7 - k : 9 - k] for c in range(3)]
    for c in range(3):
        xc_ref[c] = rows(xc[c])
        rc_ref[c] = rows(r[c])
        wc_ref[c] = rows(w[c])
        pco_ref[c] = rows(pc[c][3:13])

    m = tiles(me[...])
    order = [0] + [i for i in range(1, 9) for _ in range(2)] + [9]
    v = [spread(e[c], order) for c in range(3)]
    aw = operate(v, m, 1)
    low = inverse(m[0:3], 1, GAIN_F)
    high = inverse(m[14:17], 1, GAIN_F)
    p = [jnp.concatenate([low[c], tiles(p_ref[c]), high[c]], 0) for c in range(3)]
    r = [tiles(re[c]) - aw[c] for c in range(3)]
    start = FIRST_F / GAIN_F
    w = [p[c] * r[c] * start for c in range(3)]
    x = [tiles(x_ref[c]) + v[c][7:11] + w[c][6:10] for c in range(3)]
    aw = operate(w, m[1:16], 1)
    r = [trim(r[c]) - aw[c] for c in range(3)]
    w = [NOW_F * trim(w[c]) + p[c][1:15] * r[c] for c in range(3)]
    x = [x[c] + w[c][5:9] for c in range(3)]
    aw = operate(w, m[2:15], 1)
    r = [trim(r[c]) - aw[c] for c in range(3)]
    f = [
        jnp.concatenate([strided(f_ref, c, z).reshape(1, 4, 8, 128) for z in range(4)], 0)
        for c in range(3)
    ]
    whole = sum(jnp.sum(x[c] * (f[c] + r[c][4:8])) for c in range(3))
    w = [p[c][2:14] * r[c] * start for c in range(3)]
    x = [x[c] + w[c][4:8] for c in range(3)]
    aw = operate(w, m[3:14], 1)
    r = [trim(r[c]) - aw[c] for c in range(3)]
    w = [NOW_F * trim(w[c]) + p[c][3:13] * r[c] for c in range(3)]
    aw = operate(w, m[4:13], 1)
    for c in range(3):
        xo_ref[c] = rows(x[c] + w[c][3:7])
        done = trim(r[c]) - aw[c]
        ro_ref[c] = rows(done[1:7])
        rc = pair_cells(done) * 0.5
        far_ref[2 * c : 2 * c + 1] = rows(pack(rc[0:1], rc[1:2]))
        far_ref[2 * c + 1 : 2 * c + 2] = rows(pack(rc[2:3], rc[3:4]))
    cmo_ref[...] = cm[3:14]
    at = lanes((1, 128))
    line = jnp.where(at == 0, whole, 0.0) + jnp.where(at == 1, part, 0.0)
    sum_ref[...] = jnp.broadcast_to(line[None], sum_ref.shape)


def late_kernel(cm_ref, pc_ref, xc_ref, rc_ref, wc_ref, coarse_ref):
    mc = tiles(cm_ref[...])
    pc = [tiles(pc_ref[c]) for c in range(3)]
    xc = [tiles(xc_ref[c]) for c in range(3)]
    r = [tiles(rc_ref[c]) for c in range(3)]
    w = [tiles(wc_ref[c]) for c in range(3)]
    for k in range(5, 8):
        aw = operate(w, mc[k - 3 : 14 - k], 2)
        r = [trim(r[c]) - aw[c] for c in range(3)]
        now, gain = STEPS_C[k - 1]
        w = [now * trim(w[c]) + gain * (pc[c][k - 3 : 13 - k] * r[c]) for c in range(3)]
        xc = [xc[c] + w[c][7 - k : 9 - k] for c in range(3)]
    col = lax.broadcasted_iota(jnp.int32, (128, 64), 1)
    row = lax.broadcasted_iota(jnp.int32, (128, 64), 0)
    pick = jnp.where(row == 2 * col + 1, 1.0, 0.0).astype(jnp.float32)
    for c in range(3):
        solved = jnp.dot(
            xc[c].reshape(32, 128), pick,
            precision=lax.Precision.HIGHEST, preferred_element_type=jnp.float32,
        )
        for z in range(2):
            for t in range(2):
                at = 16 * z + 8 * t
                coarse_ref[c, z, pl.ds(t, 8, stride=2), :] = solved[at : at + 8]


def third_kernel(
    top, scale, x_ref, r_ref, own, m_ref, p_ref, cm_ref, pc_ref, sums, a2, b2, out_ref, sum_ref, cf
):
    for c in range(3):
        cf[c, 2:4] = own[2 * c : 2 * c + 2]

    def second(up, down):
        for c in range(3):
            cf[c, 4:6] = up[2 * c : 2 * c + 2]
            cf[c, 0:2] = down[2 * c : 2 * c + 2]

    place = lax.axis_index("slab")
    by_side(half(place, 2), second, a2, b2)
    even = lanes((16, 128)) % 2 == 0

    @pl.when(place == 1)
    def _():
        for c in range(3):
            cf[c, 0] = jnp.zeros((16, 128), jnp.float32)
            cf[c, 1] = jnp.where(even, 0.0, b2[2 * c])

    @pl.when(place == top - 1)
    def _():
        for c in range(3):
            cf[c, 4] = jnp.where(even, b2[2 * c + 1], 0.0)
            cf[c, 5] = jnp.zeros((16, 128), jnp.float32)

    added = jnp.sum(sums[...], axis=0)
    for k in range(2):
        sum_ref[k] = jnp.sum(jnp.where(lanes((1, 128)) == k, added, 0.0)) * scale[k]
    mc = tiles(cm_ref[...])
    pc = [tiles(pc_ref[c]) for c in range(3)]
    r = []
    for c in range(3):
        near = tiles(cf[c])
        far = pltpu.roll(near, 127, 3)
        parts = [t[i : i + 1] for i in range(6) for t in (near, far)]
        r.append(jnp.concatenate(parts[1:11], 0))
    w = [pc[c] * r[c] * FIRST_C for c in range(3)]
    e = [w[c][3:7] for c in range(3)]
    for k in range(1, 4):
        aw = operate(w, mc[k : 11 - k], 2)
        r = [trim(r[c]) - aw[c] for c in range(3)]
        now, gain = STEPS_C[k - 1]
        w = [now * trim(w[c]) + gain * (pc[c][k : 10 - k] * r[c]) for c in range(3)]
        e = [e[c] + w[c][3 - k : 7 - k] for c in range(3)]

    m = tiles(m_ref[3:10])
    order = [0, 0, 1, 1, 2, 2, 3, 3]
    v = [spread(e[c], order) for c in range(3)]
    aw = operate(v, m, 1)
    p = [tiles(p_ref[c, 3:9]) for c in range(3)]
    r = [tiles(r_ref[c]) - aw[c] for c in range(3)]
    w = [p[c] * r[c] * (FIRST_F / GAIN_F) for c in range(3)]
    aw = operate(w, m[1:6], 1)
    for c in range(3):
        after = r[c][1:5] - aw[c]
        x = tiles(x_ref[c]) + v[c][2:6] + (1.0 + NOW_F) * w[c][1:5] + p[c][1:5] * after
        for z in range(4):
            for t in range(4):
                out_ref[c, z, pl.ds(t, 8, stride=4), :] = x[z, t]


def call(kernel, outs, scratch, *args, small=(), flops=1 << 22):
    places = [pltpu.SMEM if i in small else pltpu.VMEM for i in range(len(outs))]
    return pl.pallas_call(
        kernel,
        out_shape=[jax.ShapeDtypeStruct(s, jnp.float32) for s in outs],
        in_specs=[pl.BlockSpec(memory_space=pltpu.VMEM)] * len(args),
        out_specs=[pl.BlockSpec(memory_space=place) for place in places],
        scratch_shapes=[pltpu.VMEM(s, jnp.float32) for s in scratch],
        compiler_params=pltpu.CompilerParams(vmem_limit_bytes=16 << 20),
        cost_estimate=pl.CostEstimate(flops=flops, bytes_accessed=1 << 20, transcendentals=0),
    )(*args)


def half(i, distance):
    if distance == 3:
        i = i + 3 * (i % 3) * (2 - i % 3)
    return (i // distance) % 2


def swap(x, distance, second, extra=(), axis="slab"):
    n = lax.axis_size(axis)
    pairs = list(extra)
    for i in range(n - distance):
        if half(i, distance) == second:
            pairs += [(i, i + distance), (i + distance, i)]
    return lax.ppermute(x, axis, pairs)


def shift(x, by, axis="slab"):
    n = lax.axis_size(axis)
    return lax.ppermute(x, axis, [(i, (i + by) % n) for i in range(n)])


def cycles(force, modulus):
    n = lax.axis_size("slab")
    top = n - 1
    if half(top, 3) != 1 or half(top - 2, 3) != 1 or half(top, 2) != 1:
        raise ValueError("slab count")
    block = jnp.concatenate([force.reshape(12, 32, 128), modulus], 0)
    a = shift(block, -1)
    b = shift(block, 1)
    s = lax.ppermute(modulus[3:4], "slab", [(i, i + 2) for i in range(n - 2)])
    x, r, m, p, cf, cm, send_a, send_b, far = call(
        functools.partial(first_kernel, top),
        [
            (3, 4, 32, 128), (3, 8, 32, 128), (13, 32, 128), (3, 12, 32, 128), (3, 4, 16, 128),
            (6, 16, 128), (17, 32, 128), (17, 32, 128), (18, 16, 128),
        ],
        [(3, 12, 32, 128)],
        force, modulus, a, b, s,
    )
    got = [shift(send_b, -1), shift(send_a, 1)]
    got += [swap(far, 3, 0), swap(far, 3, 1, ((0, 2), (top, top - 2)))]
    x, r, far, cm, pc, xc, rc, wc, part = call(
        functools.partial(second_kernel, top),
        [
            (3, 4, 32, 128), (3, 6, 32, 128), (6, 16, 128), (11, 16, 128), (3, 10, 16, 128),
            (3, 2, 16, 128), (3, 8, 16, 128), (3, 8, 16, 128), (n, 1, 128),
        ],
        [(3, 16, 32, 128), (17, 32, 128), (3, 16, 16, 128), (17, 16, 128)],
        force, x, r, m, p, cf, cm, *got,
    )
    got = [swap(far, 2, 0), swap(far, 2, 1, ((0, 1), (top, top - 1)))]
    sums = lax.all_to_all(part, "slab", 0, 0, tiled=True)
    (coarse,) = call(late_kernel, [(3, 2, 16, 64)], [], cm, pc, xc, rc, wc)
    cells = float(modulus.size * n)
    angle = math.acosh(RATIO_C)
    part_way = math.cosh(CDEG * angle)
    full = math.cosh(2 * CDEG * angle)
    scale = (1.0 / cells, 2.0 * part_way * part_way / full / 4.0 / (cells / 8.0))
    fine, total = call(
        functools.partial(third_kernel, top, scale),
        [(3, 4, 32, 128), (2,)],
        [(3, 6, 16, 128)],
        x, r, far, m, p, cm, pc, sums, *got, small=(1,),
    )
    return fine, coarse, total


def solution(mesh):
    return jax.shard_map(
        cycles,
        mesh=mesh,
        in_specs=(P(None, "slab", None, "sample"), P("slab", None, "sample")),
        out_specs=(P(None, "slab", None, "sample"), P(None, "slab", None, "sample"), P("sample")),
        check_vma=False,
    )
```
